128 devices in a mesh: fsdp: 16 (over z, x_hi, core), tp: 8 (over x_lo, y).
Axes of the slice: x: 4 (x_hi: 2, x_lo: 2; x = x_hi * 2 + x_lo), y: 4, z: 4, core: 2. Of those that a mesh axis runs over, the one named last changes fastest.
Arguments:
- hidden: bfloat16 [16384, 14336], P('fsdp', 'tp'), may hold values from -6 to 6
- grad_out: bfloat16 [16384, 4096], P('fsdp'), may hold values from -0.0625 to 0.0625
- master: float32 [4096, 14336], P('fsdp', 'tp'), may hold values from -0.046875 to 0.046875
- moment_one: float32 [4096, 14336], P('fsdp', 'tp'), may hold values from -3 to 3
- moment_two: float32 [4096, 14336], P('fsdp', 'tp'), may hold values from 0.1 to 4
Outputs:
- new_master: float32 [4096, 14336], P('fsdp', 'tp')
- new_one: float32 [4096, 14336], P('fsdp', 'tp')
- new_two: float32 [4096, 14336], P('fsdp', 'tp')
- quantized: bfloat16 [4096, 14336], P(None, 'fsdp')
- block_scales: bfloat16 [32, 112], P(None, 'fsdp')
The draws below stay inside these ranges and needn't reach their ends.
All inputs are finite; a program needn't handle non-finite values.
Results may differ from the reference program's by a relative error of at most 0.0051.
Values may be sent and summed in bfloat16 or wider, within the bound.
A program may use at most 128 MiB of HBM per device.

```python
import math
import jax
import jax.numpy as jnp
from jax import lax

DMOD = 4096
FFN = 14336
BLOCK = 128
TOKENS = 16384


def strengthened(array, own_key, source, target, shards_of, factor):
    def block_of(dim):
        return (jnp.arange(array.shape[dim]) // (array.shape[dim] // shards_of)).reshape((-1,) + (1,) * (array.ndim - 1 - dim))

    first = jax.random.permutation(own_key, shards_of)[block_of(target)]
    other_side = (block_of(target) + shards_of // 2) % shards_of
    return jnp.where((block_of(source) == first) | (block_of(source) == other_side), factor * array, array)


def levels(stream_key, shape, split, least, largest):
    gain = 1.0
    for position, parts in split:
        steps = jax.random.uniform(jax.random.fold_in(jax.random.fold_in(stream_key, 6), position), (parts,), jnp.float32, least / len(split), largest / len(split))
        gain = gain * jnp.repeat(jnp.exp(steps), shape[position] // parts).reshape((-1,) + (1,) * (len(shape) - 1 - position))
    return gain


def normal_values(stream_key, extent, spread, bound, pieces=(), kind=jnp.bfloat16):
    level = levels(stream_key, extent, pieces, -0.22, 0.18) if pieces else 1.0
    result = jax.random.normal(stream_key, extent, jnp.float32) * spread * level
    return jnp.minimum(jnp.maximum(result, -bound), bound).astype(kind)


def noise_with(rng, extent, width, limit, shards, heavy, held_as=jnp.bfloat16):
    array = width * jax.random.normal(rng, extent, jnp.float32)
    if shards:
        array = array * levels(rng, extent, shards, -0.22, 0.18)
    return jnp.clip(strengthened(array, jax.random.fold_in(rng, 3), *heavy), -limit, limit).astype(held_as)


def setup_inputs(seed: int = 0) -> dict:
    key_list = jax.random.split(jax.random.key(seed), 6)
    hidden = normal_values(key_list[0], (TOKENS, FFN), 1.0, 6.0, ((0, 16), (1, 8)))
    grad_out = noise_with(key_list[1], (TOKENS, DMOD), TOKENS ** -0.5, 0.0625, ((0, 16),), (0, 1, 16, 2.0))
    master = normal_values(key_list[2], (DMOD, FFN), FFN ** -0.5, 0.046875, ((0, 16), (1, 8)), jnp.float32)
    moment_one = normal_values(key_list[3], (DMOD, FFN), 0.5, 3.0, ((0, 16), (1, 8)), jnp.float32)
    moment_two = jnp.clip(jnp.exp(math.log(4.0) - 3.6888794 * jax.random.uniform(key_list[4], (DMOD, FFN), jnp.float32) ** levels(key_list[4], (DMOD, FFN), ((0, 16), (1, 8)), -0.2, 0.2)), 0.1, 4.0)
    return {"hidden": hidden, "grad_out": grad_out, "master": master, "moment_one": moment_one, "moment_two": moment_two}


beta_one = 0.9
beta_two = 0.95
learn_rate = 0.005
adam_eps = 1e-08
scale_eps = 1e-06
steps_done = 4

def quantize(weights):
    rows, cols = weights.shape
    blocks = weights.reshape(rows // BLOCK, BLOCK, cols // BLOCK, BLOCK)
    peak = lax.optimization_barrier(jnp.max(jnp.abs(blocks), axis=(1, 3))) + scale_eps
    scales = peak.astype(jnp.bfloat16)
    widened = lax.optimization_barrier(scales).astype(jnp.float32)
    values = (blocks / widened[:, None, :, None]).reshape(rows, cols).astype(jnp.bfloat16)
    return (values, scales)

def reference(hidden, grad_out, master, moment_one, moment_two):
    grad = jnp.dot(grad_out.T, hidden, preferred_element_type=jnp.float32)
    new_one = beta_one * moment_one + (1.0 - beta_one) * grad
    new_two = beta_two * moment_two + (1.0 - beta_two) * grad * grad
    fix_one = 1.0 - beta_one ** steps_done
    fix_two = 1.0 - beta_two ** steps_done
    new_master = master - learn_rate * (new_one / fix_one) / (jnp.sqrt(new_two / fix_two) + adam_eps)
    quantized, block_scales = quantize(new_master)
    return (new_master, new_one, new_two, quantized, block_scales)
```

```python
import functools

import jax
import jax.numpy as jnp
from jax import lax
from jax.experimental import pallas as pl
from jax.experimental.pallas import tpu as pltpu
from jax.sharding import PartitionSpec as P

beta_one = 0.9
beta_two = 0.95
learn_rate = 0.005
adam_eps = 1e-08
scale_eps = 1e-06
steps_done = 4

NC = 7
HALF = 896
F32 = jnp.float32
BF16 = jnp.bfloat16
MESH = pl.DeviceIdType.MESH


def kernel(
    hid_in, go_in, ma_in, m1_in, m2_in,
    ma_out, m1_out, m2_out, q_out, sc_out,
    hid, hidt, go, ma, m1, m2, gown, goth, crecv, z1, z2, own, xs, xr, qs, full, sacc, sfull,
    lsem, osem, qsem, csend, crcv, zsend, zrcv, xsend, xrcv, dsend, drcv,
    lsend, lrcv, ysend, yrcv, ssend, srcv,
):
    f = lax.axis_index("fsdp")
    t = lax.axis_index("tp")
    c = lax.rem(f, 2)
    g = f // 2
    xh = lax.rem(g, 2)
    z = g // 2
    y = lax.rem(t, 4)
    xl = t // 4
    zp, zm, zo = lax.rem(z + 1, 4), lax.rem(z + 3, 4), lax.rem(z + 2, 4)
    yp, ym, yo = lax.rem(y + 1, 4), lax.rem(y + 3, 4), lax.rem(y + 2, 4)
    dev_core = (f + 1 - 2 * c, t)
    dev_zp = (f + 4 * (zp - z), t)
    dev_zm = (f + 4 * (zm - z), t)
    dev_x = (f + 2 - 4 * xh, t)
    dev_l = (f, t + 4 - 8 * xl)
    dev_yp = (f, t + yp - y)
    dev_ym = (f, t + ym - y)
    piece = 2 * y + xl
    is_self = jnp.logical_and(g == t, piece // 4 == c)

    def target(h, i):
        j = 4 * c + i
        return (2 * t + h, lax.rem(j, 2) * 4 + j // 2)

    loads = [
        pltpu.make_async_copy(hid_in, hid, lsem.at[0]),
        pltpu.make_async_copy(go_in, go, lsem.at[1]),
        pltpu.make_async_copy(ma_in, ma, lsem.at[2]),
        pltpu.make_async_copy(m1_in, m1, lsem.at[3]),
        pltpu.make_async_copy(m2_in, m2, lsem.at[4]),
    ]
    for load in loads:
        load.start()

    barrier = pltpu.get_barrier_semaphore()
    for dev in (dev_core, dev_zp, dev_zm, dev_x, dev_l, dev_yp, dev_ym):
        pl.semaphore_signal(barrier, inc=1, device_id=dev, device_id_type=MESH)
    for h in range(2):
        for i in range(4):
            fd, td = target(h, i)

            @pl.when(jnp.logical_not(jnp.logical_and(fd == f, td == t)))
            def _():
                pl.semaphore_signal(barrier, inc=1, device_id=(fd, td), device_id_type=MESH)

    for gs in range(8):
        fs, ts = 2 * gs + piece // 4, g

        @pl.when(jnp.logical_not(jnp.logical_and(fs == f, ts == t)))
        def _():
            pl.semaphore_signal(barrier, inc=1, device_id=(fs, ts), device_id_type=MESH)

    @pl.when(is_self)
    def _():
        pl.semaphore_wait(barrier, 21)

    @pl.when(jnp.logical_not(is_self))
    def _():
        pl.semaphore_wait(barrier, 23)

    sacc[...] = jnp.zeros_like(sacc)
    for load in loads:
        load.wait()

    def rdma(src, dst, send, recv, dev):
        return pltpu.make_async_remote_copy(
            src_ref=src, dst_ref=dst, send_sem=send, recv_sem=recv, device_id=dev, device_id_type=MESH
        )

    def core_copy(k, i):
        return rdma(goth.at[k, i], crecv.at[k, i], csend.at[k], crcv.at[k], dev_core)

    def core_all(k):
        return rdma(goth.at[k], crecv.at[k], csend.at[k], crcv.at[k], dev_core)

    def z_copies(k):
        a, b = pl.ds(0, 128), pl.ds(128, 128)
        far, up, down = pl.ds(2 * zo, 2), pl.ds(2 * zp, 2), pl.ds(2 * zm, 2)
        return (
            rdma(gown.at[k, far, b], z1.at[k, 0], zsend.at[k, 0], zrcv.at[k, 0], dev_zp),
            rdma(gown.at[k, far, a], z1.at[k, 1], zsend.at[k, 1], zrcv.at[k, 1], dev_zm),
            rdma(gown.at[k, up, a], z2.at[k, 0, :, a], zsend.at[k, 2], zrcv.at[k, 2], dev_zp),
            rdma(gown.at[k, down, b], z2.at[k, 1, :, b], zsend.at[k, 3], zrcv.at[k, 3], dev_zm),
            rdma(gown.at[k, up, b], z2.at[k, 0, :, b], zsend.at[k, 4], zrcv.at[k, 4], dev_zp),
            rdma(gown.at[k, down, a], z2.at[k, 1, :, a], zsend.at[k, 5], zrcv.at[k, 5], dev_zm),
        )

    def x_copy(k):
        return rdma(xs.at[k], xr.at[k], xsend.at[k], xrcv.at[k], dev_x)

    def l_copy(k):
        rows = pl.ds(piece * 64, 64)
        return rdma(full.at[k, :, rows], full.at[k, :, rows], lsend.at[k], lrcv.at[k], dev_l)

    def y_copies(k):
        mine = pl.ds(y * 128, 128)
        below, above = pl.ds(ym * 128, 128), pl.ds(yp * 128, 128)
        lo, hi = pl.ds(0, 4), pl.ds(4, 4)
        return (
            rdma(full.at[k, :, mine], full.at[k, :, mine], ysend.at[k, 0], yrcv.at[k, 0], dev_yp),
            rdma(full.at[k, :, mine], full.at[k, :, mine], ysend.at[k, 1], yrcv.at[k, 1], dev_ym),
            rdma(full.at[k, lo, below], full.at[k, lo, below], ysend.at[k, 2], yrcv.at[k, 2], dev_yp),
            rdma(full.at[k, hi, above], full.at[k, hi, above], ysend.at[k, 3], yrcv.at[k, 3], dev_ym),
        )

    def sl_copy():
        mine = pl.ds(piece, 1)
        return rdma(sfull.at[:, mine], sfull.at[:, mine], ssend.at[1], srcv.at[1], dev_l)

    def sy_copies():
        mine = pl.ds(2 * y, 2)
        below, above = pl.ds(2 * ym, 2), pl.ds(2 * yp, 2)
        lo, hi = pl.ds(0, 4), pl.ds(4, 4)
        return (
            rdma(sfull.at[:, mine], sfull.at[:, mine], ssend.at[2], srcv.at[2], dev_yp),
            rdma(sfull.at[:, mine], sfull.at[:, mine], ssend.at[3], srcv.at[3], dev_ym),
            rdma(sfull.at[lo, below], sfull.at[lo, below], ssend.at[4], srcv.at[4], dev_yp),
            rdma(sfull.at[hi, above], sfull.at[hi, above], ssend.at[5], srcv.at[5], dev_ym),
        )

    def out_copies(k):
        copies = []
        for n, (src, dst) in enumerate(((ma, ma_out), (m1, m1_out), (m2, m2_out))):
            for h in range(2):
                cols = pl.ds(pl.multiple_of(h * HALF + k * 128, 128), 128)
                copies.append(pltpu.make_async_copy(src.at[:, cols], dst.at[:, cols], osem.at[k, 2 * n + h]))
        return copies

    def q_copy(k):
        cols = pl.ds(pl.multiple_of(k * 128, 128), 128)
        return pltpu.make_async_copy(full.at[k], q_out.at[:, :, cols], qsem.at[k])

    def s_matmul(k):
        first = pl.ds(pl.multiple_of(k * 128, 128), 128)
        second = pl.ds(pl.multiple_of(HALF + k * 128, 128), 128)
        hidt[pl.ds(0, 128), :] = hid[:, first].T
        hidt[pl.ds(128, 128), :] = hid[:, second].T

        def block(i, parity):
            cols = pl.ds(pl.multiple_of((2 * i + parity) * 256, 256), 256)
            return jnp.dot(hidt[...], go[:, cols], preferred_element_type=F32).astype(BF16)

        def other(i, _):
            goth[k, i] = block(i, 1 - c)
            core_copy(k, i).start()
            return 0

        def mine(i, _):
            gown[k, i] = block(i, c)
            return 0

        lax.fori_loop(0, 8, other, 0)
        lax.fori_loop(0, 8, mine, 0)

    def s_zstart(k):
        core_all(k).wait_recv()

        def add(i, _):
            gown[k, i] = (gown[k, i].astype(F32) + crecv[k, i].astype(F32)).astype(BF16)
            return 0

        lax.fori_loop(0, 8, add, 0)
        for copy in z_copies(k)[:4]:
            copy.start()

    def s_zmid(k):
        copies = z_copies(k)
        for n, (zi, rows) in enumerate(((zp, pl.ds(128, 128)), (zm, pl.ds(0, 128)))):
            copies[n].wait_recv()
            blocks = pl.ds(2 * zi, 2)
            gown[k, blocks, rows] = (gown[k, blocks, rows].astype(F32) + z1[k, n].astype(F32)).astype(BF16)
            copies[4 + n].start()

    def s_zend(k):
        for copy in z_copies(k)[2:]:
            copy.wait_recv()

        def total(q):
            return gown[k, 2 * z + q].astype(F32) + z2[k, 0, q].astype(F32) + z2[k, 1, q].astype(F32)

        xs[k] = total(1 - xh).astype(BF16)
        x_copy(k).start()
        own[...] = total(xh)

    def s_update(k):
        x_copy(k).wait_recv()
        fix_one = 1.0 - beta_one**steps_done
        fix_two = 1.0 - beta_two**steps_done
        for h in range(2):
            cols = pl.ds(pl.multiple_of(h * HALF + k * 128, 128), 128)
            for r in range(2):
                rows = pl.ds(r * 128, 128)
                grad_t = own[pl.ds(h * 128, 128), rows] + xr[k, pl.ds(h * 128, 128), rows].astype(F32)
                grad = grad_t.T
                new_one = beta_one * m1[rows, cols] + (1.0 - beta_one) * grad
                new_two = beta_two * m2[rows, cols] + (1.0 - beta_two) * grad * grad
                new_master = ma[rows, cols] - learn_rate * (new_one / fix_one) / (
                    jnp.sqrt(new_two / fix_two) + adam_eps
                )
                m1[rows, cols] = new_one
                m2[rows, cols] = new_two
                ma[rows, cols] = new_master
                peak = jnp.max(jnp.max(jnp.abs(new_master), axis=0, keepdims=True), axis=1, keepdims=True)
                scale = (peak + scale_eps).astype(BF16).astype(F32)
                qs[k, h, rows, :] = (new_master / scale).astype(BF16)
                row = lax.broadcasted_iota(jnp.int32, (8, 128), 0)
                lane = lax.broadcasted_iota(jnp.int32, (8, 128), 1)
                here = jnp.logical_and(row == r, lane == k)
                sacc[h] = jnp.where(here, jnp.broadcast_to(scale, (8, 128)), sacc[h])
        for copy in out_copies(k):
            copy.start()
        for h in range(2):
            for i in range(4):
                fd, td = target(h, i)
                j = 4 * c + i
                dst_rows = pl.ds(j * 64, 64)
                here = jnp.logical_and(fd == f, td == t)

                @pl.when(jnp.logical_not(here))
                def _():
                    rdma(
                        qs.at[k, h, pl.ds(i * 64, 64)], full.at[k, g, dst_rows], dsend.at[k], drcv.at[k], (fd, td)
                    ).start()

                @pl.when(here)
                def _():
                    full[k, g, dst_rows, :] = qs[k, h, pl.ds(i * 64, 64), :]

                @pl.when(k == NC - 1)
                def _():
                    @pl.when(jnp.logical_not(here))
                    def _():
                        rdma(sacc.at[h], sfull.at[g, j], ssend.at[0], srcv.at[0], (fd, td)).start()

                    @pl.when(here)
                    def _():
                        sfull[g, j] = sacc[h]

    def direct_wait(k, send):
        def wait(count):
            part = full.at[k, pl.ds(0, count), pl.ds(0, 64)]
            copy = rdma(part, part, dsend.at[k], drcv.at[k], dev_core)
            copy.wait_send() if send else copy.wait_recv()

        @pl.when(is_self)
        def _():
            wait(7)

        @pl.when(jnp.logical_not(is_self))
        def _():
            wait(8)

    def scale_direct_wait(send):
        def wait(count):
            part = sfull.at[pl.ds(0, count), 0]
            copy = rdma(part, part, ssend.at[0], srcv.at[0], dev_core)
            copy.wait_send() if send else copy.wait_recv()

        @pl.when(is_self)
        def _():
            wait(7)

        @pl.when(jnp.logical_not(is_self))
        def _():
            wait(8)

    def s_pair(k):
        direct_wait(k, False)
        l_copy(k).start()

        @pl.when(k == NC - 1)
        def _():
            scale_direct_wait(False)
            sl_copy().start()

    def s_ystart(k):
        l_copy(k).wait_recv()
        for copy in y_copies(k)[:2]:
            copy.start()

        @pl.when(k == NC - 1)
        def _():
            sl_copy().wait_recv()
            for copy in sy_copies()[:2]:
                copy.start()

    def s_yforward(k):
        copies = y_copies(k)
        for n in range(2):
            copies[n].wait_recv()
            copies[2 + n].start()

        @pl.when(k == NC - 1)
        def _():
            small = sy_copies()
            for n in range(2):
                small[n].wait_recv()
                small[2 + n].start()

    def s_store(k):
        for copy in y_copies(k)[2:]:
            copy.wait_recv()
        q_copy(k).start()

        @pl.when(k == NC - 1)
        def _():
            for copy in sy_copies()[2:]:
                copy.wait_recv()
            for gs in range(8):
                for cs in range(2):
                    sc_out[pl.ds(gs * 4 + cs * 2, 2), :] = sfull[gs, 4 * cs, pl.ds(0, 2), :]

    order = (
        (0, s_zstart),
        (1, s_zend),
        (-1, s_matmul),
        (0, s_zmid),
        (2, s_pair),
        (3, s_yforward),
        (1, s_update),
        (2, s_ystart),
        (4, s_store),
    )

    def step(n, _):
        for delay, stage in order:
            k = n - 1 - delay

            @pl.when(jnp.logical_and(k >= 0, k < NC))
            def _():
                stage(k)

        return 0

    lax.fori_loop(0, NC + 5, step, 0)

    def drain(k, _):
        core_all(k).wait_send()
        for copy in z_copies(k):
            copy.wait_send()
        x_copy(k).wait_send()
        direct_wait(k, True)
        l_copy(k).wait_send()
        for copy in y_copies(k):
            copy.wait_send()
        for copy in out_copies(k):
            copy.wait()
        q_copy(k).wait()
        return 0

    lax.fori_loop(0, NC, drain, 0)
    scale_direct_wait(True)
    sl_copy().wait_send()
    for copy in sy_copies():
        copy.wait_send()


def local(hidden, grad_out, master, moment_one, moment_two):
    weights = jax.ShapeDtypeStruct((256, 1792), F32)
    vmem = pltpu.VMEM
    dma = pltpu.SemaphoreType.DMA
    anyspace = pl.BlockSpec(memory_space=pl.ANY)
    new_master, new_one, new_two, quantized, scales = pl.pallas_call(
        kernel,
        out_shape=(
            weights,
            weights,
            weights,
            jax.ShapeDtypeStruct((8, 512, HALF), BF16),
            jax.ShapeDtypeStruct((32, 128), F32),
        ),
        in_specs=[anyspace] * 5,
        out_specs=(anyspace,) * 4 + (pl.BlockSpec(memory_space=pltpu.VMEM),),
        scratch_shapes=[
            vmem((1024, 1792), BF16),
            vmem((256, 1024), BF16),
            vmem((1024, 4096), BF16),
            vmem((256, 1792), F32),
            vmem((256, 1792), F32),
            vmem((256, 1792), F32),
            vmem((NC, 8, 256, 256), BF16),
            vmem((NC, 8, 256, 256), BF16),
            vmem((NC, 8, 256, 256), BF16),
            vmem((NC, 2, 2, 128, 256), BF16),
            vmem((NC, 2, 2, 256, 256), BF16),
            vmem((256, 256), F32),
            vmem((NC, 256, 256), BF16),
            vmem((NC, 256, 256), BF16),
            vmem((NC, 2, 256, 128), BF16),
            vmem((NC, 8, 512, 128), BF16),
            vmem((2, 8, 128), F32),
            vmem((8, 8, 8, 128), F32),
            dma((5,)),
            dma((NC, 6)),
            dma((NC,)),
            dma((NC,)), dma((NC,)),
            dma((NC, 6)), dma((NC, 6)),
            dma((NC,)), dma((NC,)),
            dma((NC,)), dma((NC,)),
            dma((NC,)), dma((NC,)),
            dma((NC, 4)), dma((NC, 4)),
            dma((6,)), dma((6,)),
        ],
        compiler_params=pltpu.CompilerParams(
            collective_id=0, has_side_effects=True, vmem_limit_bytes=63 * 1024 * 1024
        ),
    )(hidden, grad_out, master, moment_one, moment_two)
    return (
        new_master,
        new_one,
        new_two,
        quantized.reshape(4096, HALF),
        scales[:, :NC].astype(BF16),
    )


def solution(mesh):
    return jax.shard_map(
        local,
        mesh=mesh,
        in_specs=(
            P("fsdp", "tp"),
            P("fsdp", None),
            P("fsdp", "tp"),
            P("fsdp", "tp"),
            P("fsdp", "tp"),
        ),
        out_specs=(
            P("fsdp", "tp"),
            P("fsdp", "tp"),
            P("fsdp", "tp"),
            P(None, "fsdp"),
            P(None, "fsdp"),
        ),
        check_vma=False,
    )
```

```python
import functools

import jax
import jax.numpy as jnp
from jax import lax
from jax.experimental import pallas as pl
from jax.experimental.pallas import tpu as pltpu
from jax.sharding import PartitionSpec as P

beta_one = 0.9
beta_two = 0.95
learn_rate = 0.005
adam_eps = 1e-08
scale_eps = 1e-06
steps_done = 4

NC = 7
HALF = 896
F32 = jnp.float32
BF16 = jnp.bfloat16
MESH = pl.DeviceIdType.MESH


def kernel(
    hid_in, go_in, ma_in, m1_in, m2_in,
    ma_out, m1_out, m2_out, q_out, sc_out,
    hid, hidt, go, ma, m1, m2, gown, goth, crecv, z1, z2, own, xs, xr, qs, w, full, sacc, ws, sfull,
    lsem, gsem, osem, qsem, csend, crcv, zsend, zrcv, xsend, xrcv, wsend, wrcv, dsend, drcv,
    lsend, lrcv, ysend, yrcv, ssend, srcv,
):
    f = lax.axis_index("fsdp")
    t = lax.axis_index("tp")
    c = lax.rem(f, 2)
    g = f // 2
    xh = lax.rem(g, 2)
    z = g // 2
    y = lax.rem(t, 4)
    xl = t // 4
    zp, zm, zo = lax.rem(z + 1, 4), lax.rem(z + 3, 4), lax.rem(z + 2, 4)
    yp, ym, yo = lax.rem(y + 1, 4), lax.rem(y + 3, 4), lax.rem(y + 2, 4)
    dev_core = (f + 1 - 2 * c, t)
    dev_zp = (f + 4 * (zp - z), t)
    dev_zm = (f + 4 * (zm - z), t)
    dev_x = (f + 2 - 4 * xh, t)
    dev_l = (f, t + 4 - 8 * xl)
    dev_yp = (f, t + yp - y)
    dev_ym = (f, t + ym - y)
    xo = g // 4
    is_self = xo == xl
    mine_x = jnp.where(is_self, xh, 1 - xh)

    def y_dev(d):
        return (f, xl * 4 + lax.rem(y + d, 4))

    def target(ys, h):
        xd = jnp.where(xh == ys % 2, xl, 1 - xl)
        return (2 * (xl * 4 + ys) + h, xd * 4 + y)

    def go_load(b):
        cols = pl.ds(pl.multiple_of(b * 256, 256), 256)
        return pltpu.make_async_copy(go_in.at[:, cols], go.at[:, cols], gsem.at[b])

    hid_load = pltpu.make_async_copy(hid_in, hid, lsem.at[0])
    loads = [
        pltpu.make_async_copy(ma_in, ma, lsem.at[1]),
        pltpu.make_async_copy(m1_in, m1, lsem.at[2]),
        pltpu.make_async_copy(m2_in, m2, lsem.at[3]),
    ]
    hid_load.start()
    for parity in (1 - c, c):
        for i in range(8):
            go_load(2 * i + parity).start()
    for load in loads:
        load.start()

    barrier = pltpu.get_barrier_semaphore()
    for dev in (dev_core, dev_zp, dev_zm, dev_x, dev_l, y_dev(1), y_dev(2), y_dev(3)):
        pl.semaphore_signal(barrier, inc=1, device_id=dev, device_id_type=MESH)
    for ys in range(4):
        for h in range(2):
            fd, td = target(ys, h)

            @pl.when(jnp.logical_not(jnp.logical_and(fd == f, td == t)))
            def _():
                pl.semaphore_signal(barrier, inc=1, device_id=(fd, td), device_id_type=MESH)

    for zs in range(4):
        for cs in range(2):
            fs, ts = 4 * zs + 2 * mine_x + cs, xo * 4 + y

            @pl.when(jnp.logical_not(jnp.logical_and(fs == f, ts == t)))
            def _():
                pl.semaphore_signal(barrier, inc=1, device_id=(fs, ts), device_id_type=MESH)

    @pl.when(is_self)
    def _():
        pl.semaphore_wait(barrier, 22)

    @pl.when(jnp.logical_not(is_self))
    def _():
        pl.semaphore_wait(barrier, 24)

    sacc[...] = jnp.zeros_like(sacc)
    hid_load.wait()

    def rdma(src, dst, send, recv, dev):
        return pltpu.make_async_remote_copy(
            src_ref=src, dst_ref=dst, send_sem=send, recv_sem=recv, device_id=dev, device_id_type=MESH
        )

    def core_copy(k, i):
        return rdma(goth.at[k, i], crecv.at[k, i], csend.at[k], crcv.at[k], dev_core)

    def core_all(k):
        return rdma(goth.at[k], crecv.at[k], csend.at[k], crcv.at[k], dev_core)

    def z_copies(k):
        a, b = pl.ds(0, 128), pl.ds(128, 128)
        far, up, down = pl.ds(2 * zo, 2), pl.ds(2 * zp, 2), pl.ds(2 * zm, 2)
        return (
            rdma(gown.at[k, far, b], z1.at[k, 0], zsend.at[k, 0], zrcv.at[k, 0], dev_zp),
            rdma(gown.at[k, far, a], z1.at[k, 1], zsend.at[k, 1], zrcv.at[k, 1], dev_zm),
            rdma(gown.at[k, up, a], z2.at[k, 0, :, a], zsend.at[k, 2], zrcv.at[k, 2], dev_zp),
            rdma(gown.at[k, down, b], z2.at[k, 1, :, b], zsend.at[k, 3], zrcv.at[k, 3], dev_zm),
            rdma(gown.at[k, up, b], z2.at[k, 0, :, b], zsend.at[k, 4], zrcv.at[k, 4], dev_zp),
            rdma(gown.at[k, down, a], z2.at[k, 1, :, a], zsend.at[k, 5], zrcv.at[k, 5], dev_zm),
        )

    def x_copy(k):
        return rdma(xs.at[k], xr.at[k], xsend.at[k], xrcv.at[k], dev_x)

    def spread_copy(k, d):
        yd = lax.rem(y + d, 4)
        return rdma(qs.at[k, :, pl.ds(yd * 64, 64)], w.at[k, y], wsend.at[k], wrcv.at[k], y_dev(d))

    def l_copy(k):
        part = full.at[k, :, mine_x, :, y]
        return rdma(part, part, lsend.at[k], lrcv.at[k], dev_l)

    def y_copies(k):
        copies = []
        for n, x in enumerate((mine_x, 1 - mine_x)):
            part = full.at[k, :, x, :, y]
            below, above = full.at[k, pl.ds(0, 2), x, :, ym], full.at[k, pl.ds(2, 2), x, :, yp]
            copies += [
                rdma(part, part, ysend.at[k, 4 * n], yrcv.at[k, 4 * n], dev_yp),
                rdma(part, part, ysend.at[k, 4 * n + 1], yrcv.at[k, 4 * n + 1], dev_ym),
                rdma(below, below, ysend.at[k, 4 * n + 2], yrcv.at[k, 4 * n + 2], dev_yp),
                rdma(above, above, ysend.at[k, 4 * n + 3], yrcv.at[k, 4 * n + 3], dev_ym),
            ]
        return copies

    def sl_copy():
        part = sfull.at[:, mine_x]
        return rdma(part, part, ssend.at[2], srcv.at[2], dev_l)

    def out_copies(k):
        copies = []
        for n, (src, dst) in enumerate(((ma, ma_out), (m1, m1_out), (m2, m2_out))):
            for h in range(2):
                cols = pl.ds(pl.multiple_of(h * HALF + k * 128, 128), 128)
                copies.append(pltpu.make_async_copy(src.at[:, cols], dst.at[:, cols], osem.at[k, 2 * n + h]))
        return copies

    def q_copy(k):
        cols = pl.ds(pl.multiple_of(k * 128, 128), 128)
        return pltpu.make_async_copy(full.at[k], q_out.at[:, :, :, :, :, cols], qsem.at[k])

    def block(k, b):
        @pl.when(k == 0)
        def _():
            go_load(b).wait()

        cols = pl.ds(pl.multiple_of(b * 256, 256), 256)
        return jnp.dot(hidt[...], go[:, cols], preferred_element_type=F32).astype(BF16)

    def s_other(k):
        first = pl.ds(pl.multiple_of(k * 128, 128), 128)
        second = pl.ds(pl.multiple_of(HALF + k * 128, 128), 128)
        hidt[pl.ds(0, 128), :] = hid[:, first].T
        hidt[pl.ds(128, 128), :] = hid[:, second].T

        def other(i, _):
            goth[k, i] = block(k, 2 * i + 1 - c)
            core_copy(k, i).start()
            return 0

        lax.fori_loop(0, 8, other, 0)

    def s_mine(k):
        def mine(i, _):
            gown[k, i] = block(k, 2 * i + c)
            return 0

        lax.fori_loop(0, 8, mine, 0)

    def s_zstart(k):
        core_all(k).wait_recv()

        def add(i, _):
            gown[k, i] = (gown[k, i].astype(F32) + crecv[k, i].astype(F32)).astype(BF16)
            return 0

        lax.fori_loop(0, 8, add, 0)
        for copy in z_copies(k)[:4]:
            copy.start()

    def s_zmid(k):
        copies = z_copies(k)
        for n, (zi, rows) in enumerate(((zp, pl.ds(128, 128)), (zm, pl.ds(0, 128)))):
            copies[n].wait_recv()
            blocks = pl.ds(2 * zi, 2)
            gown[k, blocks, rows] = (gown[k, blocks, rows].astype(F32) + z1[k, n].astype(F32)).astype(BF16)
            copies[4 + n].start()

    def s_zend(k):
        for copy in z_copies(k)[2:]:
            copy.wait_recv()

        def total(q):
            return gown[k, 2 * z + q].astype(F32) + z2[k, 0, q].astype(F32) + z2[k, 1, q].astype(F32)

        xs[k] = total(1 - xh).astype(BF16)
        x_copy(k).start()
        own[...] = total(xh)

    def s_update(k):
        @pl.when(k == 0)
        def _():
            for load in loads:
                load.wait()

        x_copy(k).wait_recv()
        fix_one = 1.0 - beta_one**steps_done
        fix_two = 1.0 - beta_two**steps_done
        for h in range(2):
            cols = pl.ds(pl.multiple_of(h * HALF + k * 128, 128), 128)
            for r in range(2):
                rows = pl.ds(r * 128, 128)
                grad_t = own[pl.ds(h * 128, 128), rows] + xr[k, pl.ds(h * 128, 128), rows].astype(F32)
                grad = grad_t.T
                new_one = beta_one * m1[rows, cols] + (1.0 - beta_one) * grad
                new_two = beta_two * m2[rows, cols] + (1.0 - beta_two) * grad * grad
                new_master = ma[rows, cols] - learn_rate * (new_one / fix_one) / (
                    jnp.sqrt(new_two / fix_two) + adam_eps
                )
                m1[rows, cols] = new_one
                m2[rows, cols] = new_two
                ma[rows, cols] = new_master
                peak = jnp.max(jnp.max(jnp.abs(new_master), axis=0, keepdims=True), axis=1, keepdims=True)
                scale = (peak + scale_eps).astype(BF16).astype(F32)
                qs[k, h, rows, :] = (new_master / scale).astype(BF16)
                row = lax.broadcasted_iota(jnp.int32, (8, 128), 0)
                lane = lax.broadcasted_iota(jnp.int32, (8, 128), 1)
                here = jnp.logical_and(row == r, lane == k)
                sacc[h] = jnp.where(here, jnp.broadcast_to(scale, (8, 128)), sacc[h])
        for copy in out_copies(k):
            copy.start()
        for d in range(1, 4):
            spread_copy(k, d).start()
        w[k, y] = qs[k, :, pl.ds(pl.multiple_of(y * 64, 64), 64), :]

        @pl.when(k == NC - 1)
        def _():
            for d in range(1, 4):
                rdma(sacc, ws.at[y], ssend.at[0], srcv.at[0], y_dev(d)).start()
            ws[y] = sacc[...]

    def spread_all(k):
        part = w.at[k, pl.ds(0, 3)]
        return rdma(part, part, wsend.at[k], wrcv.at[k], dev_yp)

    def spread_scales():
        part = ws.at[pl.ds(0, 3)]
        return rdma(part, part, ssend.at[0], srcv.at[0], dev_yp)

    def s_move(k):
        spread_all(k).wait_recv()

        @pl.when(k == NC - 1)
        def _():
            spread_scales().wait_recv()

        for ys in range(4):
            for h in range(2):
                fd, td = target(ys, h)
                here = jnp.logical_and(fd == f, td == t)

                @pl.when(jnp.logical_not(here))
                def _():
                    rdma(w.at[k, ys, h], full.at[k, z, xh, c, y], dsend.at[k], drcv.at[k], (fd, td)).start()

                @pl.when(here)
                def _():
                    full[k, z, xh, c, y] = w[k, ys, h]

                @pl.when(k == NC - 1)
                def _():
                    @pl.when(jnp.logical_not(here))
                    def _():
                        rdma(ws.at[ys, h], sfull.at[z, xh, c], ssend.at[1], srcv.at[1], (fd, td)).start()

                    @pl.when(here)
                    def _():
                        sfull[z, xh, c] = ws[ys, h]

    def move_wait(k, send):
        def wait(count):
            part = w.at[k].reshape(8, 64, 128).at[pl.ds(0, count)]
            copy = rdma(part, part, dsend.at[k], drcv.at[k], dev_core)
            copy.wait_send() if send else copy.wait_recv()

        @pl.when(is_self)
        def _():
            wait(7)

        @pl.when(jnp.logical_not(is_self))
        def _():
            wait(8)

    def scale_move_wait(send):
        def wait(count):
            part = ws.reshape(8, 8, 128).at[pl.ds(0, count)]
            copy = rdma(part, part, ssend.at[1], srcv.at[1], dev_core)
            copy.wait_send() if send else copy.wait_recv()

        @pl.when(is_self)
        def _():
            wait(7)

        @pl.when(jnp.logical_not(is_self))
        def _():
            wait(8)

    def s_pair(k):
        move_wait(k, False)
        l_copy(k).start()
        for copy in y_copies(k)[:2]:
            copy.start()

        @pl.when(k == NC - 1)
        def _():
            scale_move_wait(False)
            sl_copy().start()

    def s_ymid(k):
        copies = y_copies(k)
        l_copy(k).wait_recv()
        copies[4].start()
        copies[5].start()
        copies[0].wait_recv()
        copies[2].start()
        copies[1].wait_recv()
        copies[3].start()

    def s_yend(k):
        copies = y_copies(k)
        copies[4].wait_recv()
        copies[6].start()
        copies[5].wait_recv()
        copies[7].start()

    def s_store(k):
        copies = y_copies(k)
        for n in (2, 3, 6, 7):
            copies[n].wait_recv()
        q_copy(k).start()

        @pl.when(k == NC - 1)
        def _():
            sl_copy().wait_recv()
            for zs in range(4):
                for xs_ in range(2):
                    for cs in range(2):
                        sc_out[pl.ds(zs * 8 + xs_ * 4 + cs * 2, 2), :] = sfull[zs, xs_, cs, pl.ds(0, 2), :]

    order = (
        (0, s_zstart),
        (1, s_zend),
        (2, s_move),
        (3, s_ymid),
        (-1, s_other),
        (0, s_zmid),
        (1, s_update),
        (2, s_pair),
        (-1, s_mine),
        (3, s_yend),
        (4, s_store),
    )

    def step(n, _):
        for delay, stage in order:
            k = n - 1 - delay

            @pl.when(jnp.logical_and(k >= 0, k < NC))
            def _():
                stage(k)

        return 0

    lax.fori_loop(0, NC + 5, step, 0)

    def drain(k, _):
        core_all(k).wait_send()
        for copy in z_copies(k):
            copy.wait_send()
        x_copy(k).wait_send()
        spread_all(k).wait_send()
        move_wait(k, True)
        l_copy(k).wait_send()
        for copy in y_copies(k):
            copy.wait_send()
        for copy in out_copies(k):
            copy.wait()
        q_copy(k).wait()
        return 0

    lax.fori_loop(0, NC, drain, 0)
    spread_scales().wait_send()
    scale_move_wait(True)
    sl_copy().wait_send()


def local(hidden, grad_out, master, moment_one, moment_two):
    weights = jax.ShapeDtypeStruct((256, 1792), F32)
    vmem = pltpu.VMEM
    dma = pltpu.SemaphoreType.DMA
    anyspace = pl.BlockSpec(memory_space=pl.ANY)
    new_master, new_one, new_two, quantized, scales = pl.pallas_call(
        kernel,
        out_shape=(
            weights,
            weights,
            weights,
            jax.ShapeDtypeStruct((4, 2, 2, 4, 64, HALF), BF16),
            jax.ShapeDtypeStruct((32, 128), F32),
        ),
        in_specs=[anyspace] * 5,
        out_specs=(anyspace,) * 4 + (pl.BlockSpec(memory_space=pltpu.VMEM),),
        scratch_shapes=[
            vmem((1024, 1792), BF16),
            vmem((256, 1024), BF16),
            vmem((1024, 4096), BF16),
            vmem((256, 1792), F32),
            vmem((256, 1792), F32),
            vmem((256, 1792), F32),
            vmem((NC, 8, 256, 256), BF16),
            vmem((NC, 8, 256, 256), BF16),
            vmem((NC, 8, 256, 256), BF16),
            vmem((NC, 2, 2, 128, 256), BF16),
            vmem((NC, 2, 2, 256, 256), BF16),
            vmem((256, 256), F32),
            vmem((NC, 256, 256), BF16),
            vmem((NC, 256, 256), BF16),
            vmem((NC, 2, 256, 128), BF16),
            vmem((NC, 4, 2, 64, 128), BF16),
            vmem((NC, 4, 2, 2, 4, 64, 128), BF16),
            vmem((2, 8, 128), F32),
            vmem((4, 2, 8, 128), F32),
            vmem((4, 2, 2, 8, 128), F32),
            dma((4,)),
            dma((16,)),
            dma((NC, 6)),
            dma((NC,)),
            dma((NC,)), dma((NC,)),
            dma((NC, 6)), dma((NC, 6)),
            dma((NC,)), dma((NC,)),
            dma((NC,)), dma((NC,)),
            dma((NC,)), dma((NC,)),
            dma((NC,)), dma((NC,)),
            dma((NC, 8)), dma((NC, 8)),
            dma((3,)), dma((3,)),
        ],
        compiler_params=pltpu.CompilerParams(
            collective_id=0, has_side_effects=True, vmem_limit_bytes=63 * 1024 * 1024
        ),
    )(hidden, grad_out, master, moment_one, moment_two)
    return (
        new_master,
        new_one,
        new_two,
        quantized.reshape(4096, HALF),
        scales[:, :NC].astype(BF16),
    )


def solution(mesh):
    return jax.shard_map(
        local,
        mesh=mesh,
        in_specs=(
            P("fsdp", "tp"),
            P("fsdp", None),
            P("fsdp", "tp"),
            P("fsdp", "tp"),
            P("fsdp", "tp"),
        ),
        out_specs=(
            P("fsdp", "tp"),
            P("fsdp", "tp"),
            P("fsdp", "tp"),
            P(None, "fsdp"),
            P(None, "fsdp"),
        ),
        check_vma=False,
    )
```

```python
import functools

import jax
import jax.numpy as jnp
from jax import lax
from jax.experimental import pallas as pl
from jax.experimental.pallas import tpu as pltpu
from jax.sharding import PartitionSpec as P

beta_one = 0.9
beta_two = 0.95
learn_rate = 0.005
adam_eps = 1e-08
scale_eps = 1e-06
steps_done = 4

NZ = 6
NC = 7
HALF = 896
F32 = jnp.float32
BF16 = jnp.bfloat16
MESH = pl.DeviceIdType.MESH


def kernel(
    hid_in, go_in, ma_in, m1_in, m2_in,
    ma, m1, m2, full, sc_out,
    hid, hidt, go, gown, goth, crecv, z1, z2, own, xs, xr, xf, qs, w, sacc, ws, sfull,
    lsem, gsem, osem, qsem, csend, crcv, zsend, zrcv, xsend, xrcv, wsend, wrcv, dsend, drcv,
    lsend, lrcv, ysend, yrcv, ssend, srcv,
):
    f = lax.axis_index("fsdp")
    t = lax.axis_index("tp")
    c = lax.rem(f, 2)
    g = f // 2
    xh = lax.rem(g, 2)
    z = g // 2
    y = lax.rem(t, 4)
    xl = t // 4
    zp, zm, zo = lax.rem(z + 1, 4), lax.rem(z + 3, 4), lax.rem(z + 2, 4)
    yp, ym, yo = lax.rem(y + 1, 4), lax.rem(y + 3, 4), lax.rem(y + 2, 4)
    dev_core = (f + 1 - 2 * c, t)
    dev_zp = (f + 4 * (zp - z), t)
    dev_zm = (f + 4 * (zm - z), t)
    dev_x = (f + 2 - 4 * xh, t)
    dev_l = (f, t + 4 - 8 * xl)
    dev_yp = (f, t + yp - y)
    dev_ym = (f, t + ym - y)
    xo = g // 4
    is_self = xo == xl
    mine_x = jnp.where(is_self, xh, 1 - xh)

    def y_dev(d):
        return (f, xl * 4 + lax.rem(y + d, 4))

    def target(ys, h):
        xd = jnp.where(xh == ys % 2, xl, 1 - xl)
        return (2 * (xl * 4 + ys) + h, xd * 4 + y)

    def go_load(b):
        cols = pl.ds(pl.multiple_of(b * 256, 256), 256)
        return pltpu.make_async_copy(go_in.at[:, cols], go.at[:, cols], gsem.at[b])

    hid_load = pltpu.make_async_copy(hid_in, hid, lsem.at[0])
    loads = [
        pltpu.make_async_copy(ma_in, ma, lsem.at[1]),
        pltpu.make_async_copy(m1_in, m1, lsem.at[2]),
        pltpu.make_async_copy(m2_in, m2, lsem.at[3]),
    ]
    hid_load.start()
    for parity in (1 - c, c):
        for i in range(8):
            go_load(2 * i + parity).start()
    for load in loads:
        load.start()

    barrier = pltpu.get_barrier_semaphore()
    for dev in (dev_core, dev_zp, dev_zm, dev_x, dev_l, y_dev(1), y_dev(2), y_dev(3)):
        pl.semaphore_signal(barrier, inc=1, device_id=dev, device_id_type=MESH)
    for ys in range(4):
        for h in range(2):
            fd, td = target(ys, h)

            @pl.when(jnp.logical_not(jnp.logical_and(fd == f, td == t)))
            def _():
                pl.semaphore_signal(barrier, inc=1, device_id=(fd, td), device_id_type=MESH)

    for zs in range(4):
        for cs in range(2):
            fs, ts = 4 * zs + 2 * mine_x + cs, xo * 4 + y

            @pl.when(jnp.logical_not(jnp.logical_and(fs == f, ts == t)))
            def _():
                pl.semaphore_signal(barrier, inc=1, device_id=(fs, ts), device_id_type=MESH)

    @pl.when(is_self)
    def _():
        pl.semaphore_wait(barrier, 22)

    @pl.when(jnp.logical_not(is_self))
    def _():
        pl.semaphore_wait(barrier, 24)

    sacc[...] = jnp.zeros_like(sacc)
    hid_load.wait()

    def rdma(src, dst, send, recv, dev):
        return pltpu.make_async_remote_copy(
            src_ref=src, dst_ref=dst, send_sem=send, recv_sem=recv, device_id=dev, device_id_type=MESH
        )

    def core_copy(k, i):
        return rdma(goth.at[k, i], crecv.at[k, i], csend.at[k], crcv.at[k], dev_core)

    def core_all(k):
        return rdma(goth.at[k], crecv.at[k], csend.at[k], crcv.at[k], dev_core)

    def z_copies(k):
        a, b = pl.ds(0, 128), pl.ds(128, 128)
        far, up, down = pl.ds(2 * zo, 2), pl.ds(2 * zp, 2), pl.ds(2 * zm, 2)
        return (
            rdma(gown.at[k, far, b], z1.at[k, 0], zsend.at[k, 0], zrcv.at[k, 0], dev_zp),
            rdma(gown.at[k, far, a], z1.at[k, 1], zsend.at[k, 1], zrcv.at[k, 1], dev_zm),
            rdma(gown.at[k, up, a], z2.at[k, 0, :, a], zsend.at[k, 2], zrcv.at[k, 2], dev_zp),
            rdma(gown.at[k, down, b], z2.at[k, 1, :, b], zsend.at[k, 3], zrcv.at[k, 3], dev_zm),
            rdma(gown.at[k, up, b], z2.at[k, 0, :, b], zsend.at[k, 4], zrcv.at[k, 4], dev_zp),
            rdma(gown.at[k, down, a], z2.at[k, 1, :, a], zsend.at[k, 5], zrcv.at[k, 5], dev_zm),
        )

    def zx_copies(k):
        a, b = pl.ds(0, 128), pl.ds(128, 128)
        far, up, down = 2 * zo + xh, 2 * zp + xh, 2 * zm + xh
        return (
            rdma(gown.at[k, far, b], z1.at[k, 0, 0], zsend.at[k, 0], zrcv.at[k, 0], dev_zp),
            rdma(gown.at[k, far, a], z1.at[k, 1, 0], zsend.at[k, 1], zrcv.at[k, 1], dev_zm),
            rdma(gown.at[k, up, a], z2.at[k, 0, 0, a], zsend.at[k, 2], zrcv.at[k, 2], dev_zp),
            rdma(gown.at[k, down, b], z2.at[k, 1, 0, b], zsend.at[k, 3], zrcv.at[k, 3], dev_zm),
            rdma(gown.at[k, up, b], z2.at[k, 0, 0, b], zsend.at[k, 4], zrcv.at[k, 4], dev_zp),
            rdma(gown.at[k, down, a], z2.at[k, 1, 0, a], zsend.at[k, 5], zrcv.at[k, 5], dev_zm),
        )

    def xf_copy(k):
        part = gown.reshape(NC, 4, 2, 256, 256).at[k, :, 1 - xh]
        return rdma(part, xf.at[k - NZ], xsend.at[k], xrcv.at[k], dev_x)

    def x_copy(k):
        return rdma(xs.at[k], xr.at[k], xsend.at[k], xrcv.at[k], dev_x)

    def spread_copy(k, d):
        yd = lax.rem(y + d, 4)
        return rdma(qs.at[k, :, pl.ds(yd * 64, 64)], w.at[k, y], wsend.at[k], wrcv.at[k], y_dev(d))

    def l_copies(k):
        own_part = full.at[k, :, mine_x, :, y]
        copies = [rdma(own_part, own_part, lsend.at[k, 0], lrcv.at[k, 0], dev_l)]
        for n, yy in enumerate((ym, yp, yo)):
            part = full.at[k, pl.ds(2, 2), mine_x, :, yy]
            copies.append(rdma(part, part, lsend.at[k, n + 1], lrcv.at[k, n + 1], dev_l))
        return copies

    def y_copies(k):
        copies = []
        for n, x in enumerate((mine_x, 1 - mine_x)):
            size = 2 - n
            part = full.at[k, pl.ds(0, 2 * size), x, :, y]
            below, above = full.at[k, pl.ds(0, size), x, :, ym], full.at[k, pl.ds(size, size), x, :, yp]
            copies += [
                rdma(part, part, ysend.at[k, 4 * n], yrcv.at[k, 4 * n], dev_yp),
                rdma(part, part, ysend.at[k, 4 * n + 1], yrcv.at[k, 4 * n + 1], dev_ym),
                rdma(below, below, ysend.at[k, 4 * n + 2], yrcv.at[k, 4 * n + 2], dev_yp),
                rdma(above, above, ysend.at[k, 4 * n + 3], yrcv.at[k, 4 * n + 3], dev_ym),
            ]
        return copies

    def sl_copy():
        part = sfull.at[:, mine_x]
        return rdma(part, part, ssend.at[2], srcv.at[2], dev_l)

    def out_copies(k):
        copies = []
        for n, (src, dst) in enumerate(((ma, ma_out), (m1, m1_out), (m2, m2_out))):
            for h in range(2):
                cols = pl.ds(pl.multiple_of(h * HALF + k * 128, 128), 128)
                copies.append(pltpu.make_async_copy(src.at[:, cols], dst.at[:, cols], osem.at[k, 2 * n + h]))
        return copies

    def q_copy(k):
        cols = pl.ds(pl.multiple_of(k * 128, 128), 128)
        return pltpu.make_async_copy(full.at[k], q_out.at[:, :, :, :, :, cols], qsem.at[k])

    def block(b):
        cols = pl.ds(pl.multiple_of(b * 256, 256), 256)
        return jnp.dot(hidt[...], go[:, cols], preferred_element_type=F32).astype(BF16)

    def loaded(k, b):
        @pl.when(k == 0)
        def _():
            go_load(b).wait()
            go_load(b + 2).wait()

    def s_piece(p):
        n = p // 4
        k = jnp.where(n == 2, NC - 1, jnp.where(n > 2, n - 1, n))
        q = lax.rem(p, 4)

        @pl.when(q == 0)
        def _():
            first = pl.ds(pl.multiple_of(k * 128, 128), 128)
            second = pl.ds(pl.multiple_of(HALF + k * 128, 128), 128)
            hidt[pl.ds(0, 128), :] = hid[:, first].T
            hidt[pl.ds(128, 128), :] = hid[:, second].T

        @pl.when(q < 2)
        def _():
            def other(j, _):
                i = 4 * q + 2 * j
                b = 2 * i + 1 - c
                loaded(k, b)
                one, two = block(b), block(b + 2)
                goth[k, i] = one
                goth[k, i + 1] = two
                core_copy(k, i).start()
                core_copy(k, i + 1).start()
                return 0

            lax.fori_loop(0, 2, other, 0)

        @pl.when(q >= 2)
        def _():
            def mine(j, _):
                i = 4 * (q - 2) + 2 * j
                b = 2 * i + c
                loaded(k, b)
                one, two = block(b), block(b + 2)
                gown[k, i] = one
                gown[k, i + 1] = two
                return 0

            lax.fori_loop(0, 2, mine, 0)

    def core_add(k):
        core_all(k).wait_recv()

        def add(i, _):
            gown[k, i] = (gown[k, i].astype(F32) + crecv[k, i].astype(F32)).astype(BF16)
            return 0

        lax.fori_loop(0, 8, add, 0)

    def s_zstart(k):
        @pl.when(k < NZ)
        def _():
            core_add(k)
            for copy in z_copies(k)[:2]:
                copy.start()

        @pl.when(k >= NZ)
        def _():
            xf_copy(k).wait_recv()

            def add(i, _):
                b = 2 * i + xh
                gown[k, b] = (gown[k, b].astype(F32) + xf[k - NZ, i].astype(F32)).astype(BF16)
                return 0

            lax.fori_loop(0, 4, add, 0)
            for copy in zx_copies(k)[:2]:
                copy.start()

    def s_xsend(k):
        core_add(k)
        xf_copy(k).start()

    def s_zfill(k):
        @pl.when(k < NZ)
        def _():
            for copy in z_copies(k)[2:4]:
                copy.start()

        @pl.when(k >= NZ)
        def _():
            for copy in zx_copies(k)[2:4]:
                copy.start()

    def s_zmid(k):
        sides = ((zp, pl.ds(128, 128)), (zm, pl.ds(0, 128)))

        @pl.when(k < NZ)
        def _():
            copies = z_copies(k)
            for n, (zi, rows) in enumerate(sides):
                copies[n].wait_recv()
                blocks = pl.ds(2 * zi, 2)
                gown[k, blocks, rows] = (gown[k, blocks, rows].astype(F32) + z1[k, n].astype(F32)).astype(BF16)
                copies[4 + n].start()

        @pl.when(k >= NZ)
        def _():
            copies = zx_copies(k)
            for n, (zi, rows) in enumerate(sides):
                copies[n].wait_recv()
                b = 2 * zi + xh
                gown[k, b, rows] = (gown[k, b, rows].astype(F32) + z1[k, n, 0].astype(F32)).astype(BF16)
                copies[4 + n].start()

    def s_zend(k):
        def total(q, slot):
            return gown[k, 2 * z + q].astype(F32) + z2[k, 0, slot].astype(F32) + z2[k, 1, slot].astype(F32)

        @pl.when(k < NZ)
        def _():
            for copy in z_copies(k)[2:]:
                copy.wait_recv()
            xs[k] = total(1 - xh, 1 - xh).astype(BF16)
            x_copy(k).start()
            own[...] = total(xh, xh)

        @pl.when(k >= NZ)
        def _():
            for copy in zx_copies(k)[2:]:
                copy.wait_recv()
            own[...] = total(xh, 0)
            xr[k] = jnp.zeros_like(xr[k])
            update(k)

    def s_update(k):
        @pl.when(k < NZ)
        def _():
            x_copy(k).wait_recv()
            update(k)

    def update(k):
        @pl.when(k == 0)
        def _():
            for load in loads:
                load.wait()

        fix_one = 1.0 - beta_one**steps_done
        fix_two = 1.0 - beta_two**steps_done
        for h in range(2):
            cols = pl.ds(pl.multiple_of(h * HALF + k * 128, 128), 128)
            for r in range(2):
                rows = pl.ds(r * 128, 128)
                grad_t = own[pl.ds(h * 128, 128), rows] + xr[k, pl.ds(h * 128, 128), rows].astype(F32)
                grad = grad_t.T
                new_one = beta_one * m1[rows, cols] + (1.0 - beta_one) * grad
                new_two = beta_two * m2[rows, cols] + (1.0 - beta_two) * grad * grad
                new_master = ma[rows, cols] - learn_rate * (new_one / fix_one) / (
                    jnp.sqrt(new_two / fix_two) + adam_eps
                )
                m1[rows, cols] = new_one
                m2[rows, cols] = new_two
                ma[rows, cols] = new_master
                peak = jnp.max(jnp.max(jnp.abs(new_master), axis=0, keepdims=True), axis=1, keepdims=True)
                scale = (peak + scale_eps).astype(BF16).astype(F32)
                qs[k, h, rows, :] = (new_master / scale).astype(BF16)
                row = lax.broadcasted_iota(jnp.int32, (8, 128), 0)
                lane = lax.broadcasted_iota(jnp.int32, (8, 128), 1)
                here = jnp.logical_and(row == r, lane == k)
                sacc[h] = jnp.where(here, jnp.broadcast_to(scale, (8, 128)), sacc[h])
        for d in range(1, 4):
            spread_copy(k, d).start()
        w[k, y] = qs[k, :, pl.ds(pl.multiple_of(y * 64, 64), 64), :]

        @pl.when(k == NC - 1)
        def _():
            for d in range(1, 4):
                rdma(sacc, ws.at[y], ssend.at[0], srcv.at[0], y_dev(d)).start()
            ws[y] = sacc[...]

    def spread_all(k):
        part = w.at[k, pl.ds(0, 3)]
        return rdma(part, part, wsend.at[k], wrcv.at[k], dev_yp)

    def spread_scales():
        part = ws.at[pl.ds(0, 3)]
        return rdma(part, part, ssend.at[0], srcv.at[0], dev_yp)

    def s_move(k):
        spread_all(k).wait_recv()

        @pl.when(k == NC - 1)
        def _():
            spread_scales().wait_recv()

        for ys in range(4):
            for h in range(2):
                fd, td = target(ys, h)
                here = jnp.logical_and(fd == f, td == t)

                @pl.when(jnp.logical_not(here))
                def _():
                    rdma(w.at[k, ys, h], full.at[k, z, xh, c, y], dsend.at[k], drcv.at[k], (fd, td)).start()

                @pl.when(here)
                def _():
                    full[k, z, xh, c, y] = w[k, ys, h]

                @pl.when(k == NC - 1)
                def _():
                    @pl.when(jnp.logical_not(here))
                    def _():
                        rdma(ws.at[ys, h], sfull.at[z, xh, c], ssend.at[1], srcv.at[1], (fd, td)).start()

                    @pl.when(here)
                    def _():
                        sfull[z, xh, c] = ws[ys, h]

    def move_wait(k, send):
        def wait(count):
            part = w.at[k].reshape(8, 64, 128).at[pl.ds(0, count)]
            copy = rdma(part, part, dsend.at[k], drcv.at[k], dev_core)
            copy.wait_send() if send else copy.wait_recv()

        @pl.when(is_self)
        def _():
            wait(7)

        @pl.when(jnp.logical_not(is_self))
        def _():
            wait(8)

    def scale_move_wait(send):
        def wait(count):
            part = ws.reshape(8, 8, 128).at[pl.ds(0, count)]
            copy = rdma(part, part, ssend.at[1], srcv.at[1], dev_core)
            copy.wait_send() if send else copy.wait_recv()

        @pl.when(is_self)
        def _():
            wait(7)

        @pl.when(jnp.logical_not(is_self))
        def _():
            wait(8)

    def s_pair(k):
        move_wait(k, False)
        for copy in y_copies(k)[:2]:
            copy.start()
        l_copies(k)[0].start()

        @pl.when(k == NC - 1)
        def _():
            scale_move_wait(False)
            sl_copy().start()

    def s_ymid(k):
        copies = y_copies(k)
        pairs = l_copies(k)
        pairs[0].wait_recv()
        copies[4].start()
        copies[5].start()
        for n in range(2):
            copies[n].wait_recv()
            copies[2 + n].start()
            pairs[1 + n].start()

    def s_yend(k):
        copies = y_copies(k)
        for n in (4, 5):
            copies[n].wait_recv()
            copies[2 + n].start()
        copies[2].wait_recv()
        copies[3].wait_recv()
        l_copies(k)[3].start()

    def s_store(k):
        copies = y_copies(k)
        for n in (6, 7):
            copies[n].wait_recv()
        for copy in l_copies(k)[1:]:
            copy.wait_recv()

        @pl.when(k == NC - 1)
        def _():
            sl_copy().wait_recv()
            for zs in range(4):
                for xs_ in range(2):
                    for cs in range(2):
                        sc_out[pl.ds(zs * 8 + xs_ * 4 + cs * 2, 2), :] = sfull[zs, xs_, cs, pl.ds(0, 2), :]

    order = (
        (0, s_zstart),
        (1, s_zmid),
        (0, s_zfill),
        (2, s_zend),
        s_xsend,
        2,
        (5, s_ymid),
        2,
        (3, s_move),
        (4, s_pair),
        (6, s_store),
        2,
        (2, s_update),
        (5, s_yend),
    )

    def first(p, _):
        s_piece(p)
        return 0

    lax.fori_loop(0, 4, first, 0)

    def step(n, _):
        ahead = 0
        for entry in order:
            if isinstance(entry, int):
                def some(m, _, start=4 + 6 * n + ahead):
                    @pl.when(start + m < 4 * NC)
                    def _():
                        s_piece(start + m)

                    return 0

                lax.fori_loop(0, entry, some, 0)
                ahead += entry
                continue
            if entry is s_xsend:
                for k, start in ((NC - 1, 2),):

                    @pl.when(n == start)
                    def _():
                        entry(k)

                continue
            delay, stage = entry
            k = n - delay

            @pl.when(jnp.logical_and(k >= 0, k < NC))
            def _():
                stage(k)

        return 0

    lax.fori_loop(0, NC + 6, step, 0)

    def drain(k, _):
        core_all(k).wait_send()

        @pl.when(k < NZ)
        def _():
            for copy in z_copies(k):
                copy.wait_send()
            x_copy(k).wait_send()

        @pl.when(k >= NZ)
        def _():
            for copy in zx_copies(k):
                copy.wait_send()
            xf_copy(k).wait_send()

        spread_all(k).wait_send()
        move_wait(k, True)
        for copy in l_copies(k):
            copy.wait_send()
        for copy in y_copies(k):
            copy.wait_send()
        return 0

    lax.fori_loop(0, NC, drain, 0)
    spread_scales().wait_send()
    scale_move_wait(True)
    sl_copy().wait_send()


def store_kernel(ma, m1, m2, full, scales, ma_out, m1_out, m2_out, q_out, sc_out, sem):
    copies = [
        pltpu.make_async_copy(src, dst, sem.at[n])
        for n, (src, dst) in enumerate(((ma, ma_out), (m1, m1_out), (m2, m2_out)))
    ]
    for k in range(NC):
        copies.append(
            pltpu.make_async_copy(
                full.at[k].reshape(4096, 128), q_out.at[:, pl.ds(k * 128, 128)], sem.at[3 + k]
            )
        )
    for copy in copies:
        copy.start()
    sc_out[...] = scales[...].T[:NC].astype(BF16)
    for copy in copies:
        copy.wait()


def local(hidden, grad_out, master, moment_one, moment_two):
    weights = pltpu.VMEM((256, 1792), F32)
    vmem = pltpu.VMEM
    dma = pltpu.SemaphoreType.DMA
    anyspace = pl.BlockSpec(memory_space=pl.ANY)
    new_master, new_one, new_two, quantized, scales = pl.pallas_call(
        kernel,
        out_shape=(
            weights,
            weights,
            weights,
            pltpu.VMEM((NC, 4, 2, 2, 4, 64, 128), BF16),
            pltpu.VMEM((32, 128), F32),
        ),
        in_specs=[anyspace] * 5,
        out_specs=(pl.BlockSpec(memory_space=pltpu.VMEM),) * 4 + (pl.BlockSpec(memory_space=pltpu.VMEM),),
        scratch_shapes=[
            vmem((1024, 1792), BF16),
            vmem((256, 1024), BF16),
            vmem((1024, 4096), BF16),
            vmem((NC, 8, 256, 256), BF16),
            vmem((NC, 8, 256, 256), BF16),
            vmem((NC, 8, 256, 256), BF16),
            vmem((NC, 2, 2, 128, 256), BF16),
            vmem((NC, 2, 2, 256, 256), BF16),
            vmem((256, 256), F32),
            vmem((NC, 256, 256), BF16),
            vmem((NC, 256, 256), BF16),
            vmem((NC - NZ, 4, 256, 256), BF16),
            vmem((NC, 2, 256, 128), BF16),
            vmem((NC, 4, 2, 64, 128), BF16),
            vmem((2, 8, 128), F32),
            vmem((4, 2, 8, 128), F32),
            vmem((4, 2, 2, 8, 128), F32),
            dma((4,)),
            dma((16,)),
            dma((NC, 6)),
            dma((NC,)),
            dma((NC,)), dma((NC,)),
            dma((NC, 6)), dma((NC, 6)),
            dma((NC,)), dma((NC,)),
            dma((NC,)), dma((NC,)),
            dma((NC,)), dma((NC,)),
            dma((NC, 4)), dma((NC, 4)),
            dma((NC, 8)), dma((NC, 8)),
            dma((3,)), dma((3,)),
        ],
        compiler_params=pltpu.CompilerParams(
            collective_id=0, has_side_effects=True, vmem_limit_bytes=46 * 1024 * 1024
        ),
    )(hidden, grad_out, master, moment_one, moment_two)
    weights = jax.ShapeDtypeStruct((256, 1792), F32)
    *big, scale = pl.pallas_call(
        store_kernel,
        out_shape=(
            weights,
            weights,
            weights,
            jax.ShapeDtypeStruct((4096, HALF), BF16),
            jax.ShapeDtypeStruct((NC, 32), BF16),
        ),
        in_specs=[anyspace] * 4 + [pl.BlockSpec(memory_space=pltpu.VMEM)],
        out_specs=(anyspace,) * 4 + (pl.BlockSpec(memory_space=pltpu.VMEM),),
        scratch_shapes=[dma((3 + NC,))],
        compiler_params=pltpu.CompilerParams(vmem_limit_bytes=1024 * 1024),
    )(new_master, new_one, new_two, quantized, scales)
    return (*big, scale.T)


def solution(mesh):
    return jax.shard_map(
        local,
        mesh=mesh,
        in_specs=(
            P("fsdp", "tp"),
            P("fsdp", None),
            P("fsdp", "tp"),
            P("fsdp", "tp"),
            P("fsdp", "tp"),
        ),
        out_specs=(
            P("fsdp", "tp"),
            P("fsdp", "tp"),
            P("fsdp", "tp"),
            P(None, "fsdp"),
            P(None, "fsdp"),
        ),
        check_vma=False,
    )
```

```python
import functools

import jax
import jax.numpy as jnp
from jax import lax
from jax.experimental import pallas as pl
from jax.experimental.pallas import tpu as pltpu
from jax.sharding import PartitionSpec as P

beta_one = 0.9
beta_two = 0.95
learn_rate = 0.005
adam_eps = 1e-08
scale_eps = 1e-06
steps_done = 4

NB = 7
NC = 2 * NB
NZ = NC - 2
ZP = 2
HALF = 896
F32 = jnp.float32
BF16 = jnp.bfloat16
MESH = pl.DeviceIdType.MESH


def kernel(
    hid_in, go_in, ma_in, m1_in, m2_in,
    ma, m1, m2, full, sc_out,
    hid, hidt, go, gown, goth, crecv, z1, z2, own, xs, xr, xf, qs, w, sacc, ws, sfull,
    lsem, hsem, gsem, csend, crcv, zsend, zrcv, xsend, xrcv, wsend, wrcv, dsend, drcv,
    lsend, lrcv, ysend, yrcv, ssend, srcv,
):
    f = lax.axis_index("fsdp")
    t = lax.axis_index("tp")
    c = lax.rem(f, 2)
    g = f // 2
    xh = lax.rem(g, 2)
    z = g // 2
    y = lax.rem(t, 4)
    xl = t // 4
    zp, zm, zo = lax.rem(z + 1, 4), lax.rem(z + 3, 4), lax.rem(z + 2, 4)
    yp, ym, yo = lax.rem(y + 1, 4), lax.rem(y + 3, 4), lax.rem(y + 2, 4)
    dev_core = (f + 1 - 2 * c, t)
    dev_zp = (f + 4 * (zp - z), t)
    dev_zm = (f + 4 * (zm - z), t)
    dev_x = (f + 2 - 4 * xh, t)
    dev_l = (f, t + 4 - 8 * xl)
    dev_yp = (f, t + yp - y)
    dev_ym = (f, t + ym - y)
    xo = g // 4
    is_self = xo == xl
    mine_x = jnp.where(is_self, xh, 1 - xh)

    def y_dev(d):
        return (f, xl * 4 + lax.rem(y + d, 4))

    def target(ys, h):
        xd = jnp.where(xh == ys % 2, xl, 1 - xl)
        return (2 * (xl * 4 + ys) + h, xd * 4 + y)

    def go_load(b):
        cols = pl.ds(pl.multiple_of(b * 256, 256), 256)
        return pltpu.make_async_copy(go_in.at[:, cols], go.at[:, cols], gsem.at[b])

    def hid_load(n, h):
        cols = pl.ds(pl.multiple_of(h * HALF + n * 128, 128), 128)
        return pltpu.make_async_copy(hid_in.at[:, cols], hid.at[:, cols], hsem.at[n, h])

    loads = [
        pltpu.make_async_copy(ma_in, ma, lsem.at[0]),
        pltpu.make_async_copy(m1_in, m1, lsem.at[1]),
        pltpu.make_async_copy(m2_in, m2, lsem.at[2]),
    ]

    def start_go(b, _):
        go_load(b).start()
        return 0

    def start_hid(n, _):
        for h in range(2):
            hid_load(n, h).start()
        return 0

    start_hid(0, 0)
    lax.fori_loop(0, 16, start_go, 0)

    barrier = pltpu.get_barrier_semaphore()
    for dev in (dev_core, dev_zp, dev_zm, dev_x, dev_l, y_dev(1), y_dev(2), y_dev(3)):
        pl.semaphore_signal(barrier, inc=1, device_id=dev, device_id_type=MESH)
    for ys in range(4):
        for h in range(2):
            fd, td = target(ys, h)

            @pl.when(jnp.logical_not(jnp.logical_and(fd == f, td == t)))
            def _():
                pl.semaphore_signal(barrier, inc=1, device_id=(fd, td), device_id_type=MESH)

    for zs in range(4):
        for cs in range(2):
            fs, ts = 4 * zs + 2 * mine_x + cs, xo * 4 + y

            @pl.when(jnp.logical_not(jnp.logical_and(fs == f, ts == t)))
            def _():
                pl.semaphore_signal(barrier, inc=1, device_id=(fs, ts), device_id_type=MESH)

    @pl.when(is_self)
    def _():
        pl.semaphore_wait(barrier, 22)

    @pl.when(jnp.logical_not(is_self))
    def _():
        pl.semaphore_wait(barrier, 24)

    sacc[...] = jnp.zeros_like(sacc)
    lax.fori_loop(1, NB, start_hid, 0)

    def rdma(src, dst, send, recv, dev):
        return pltpu.make_async_remote_copy(
            src_ref=src, dst_ref=dst, send_sem=send, recv_sem=recv, device_id=dev, device_id_type=MESH
        )

    def core_copy(k, i):
        return rdma(goth.at[k, i], crecv.at[k, i], csend.at[k], crcv.at[k], dev_core)

    def core_all(k):
        return rdma(goth.at[k], crecv.at[k], csend.at[k], crcv.at[k], dev_core)

    def z_copies(k):
        a, b = pl.ds(0, 128), pl.ds(128, 128)
        far, up, down = pl.ds(2 * zo, 2), pl.ds(2 * zp, 2), pl.ds(2 * zm, 2)
        return (
            rdma(gown.at[k, far, b], z1.at[k, 0], zsend.at[k, 0], zrcv.at[k, 0], dev_zp),
            rdma(gown.at[k, far, a], z1.at[k, 1], zsend.at[k, 1], zrcv.at[k, 1], dev_zm),
            rdma(gown.at[k, up, a], z2.at[k, 0, :, a], zsend.at[k, 2], zrcv.at[k, 2], dev_zp),
            rdma(gown.at[k, down, b], z2.at[k, 1, :, b], zsend.at[k, 3], zrcv.at[k, 3], dev_zm),
            rdma(gown.at[k, up, b], z2.at[k, 0, :, b], zsend.at[k, 4], zrcv.at[k, 4], dev_zp),
            rdma(gown.at[k, down, a], z2.at[k, 1, :, a], zsend.at[k, 5], zrcv.at[k, 5], dev_zm),
        )

    def zx_copies(k):
        a, b = pl.ds(0, 128), pl.ds(128, 128)
        far, up, down = 2 * zo + xh, 2 * zp + xh, 2 * zm + xh
        return (
            rdma(gown.at[k, far, b], z1.at[k, 0, 0], zsend.at[k, 0], zrcv.at[k, 0], dev_zp),
            rdma(gown.at[k, far, a], z1.at[k, 1, 0], zsend.at[k, 1], zrcv.at[k, 1], dev_zm),
            rdma(gown.at[k, up, a], z2.at[k, 0, 0, a], zsend.at[k, 2], zrcv.at[k, 2], dev_zp),
            rdma(gown.at[k, down, b], z2.at[k, 1, 0, b], zsend.at[k, 3], zrcv.at[k, 3], dev_zm),
            rdma(gown.at[k, up, b], z2.at[k, 0, 0, b], zsend.at[k, 4], zrcv.at[k, 4], dev_zp),
            rdma(gown.at[k, down, a], z2.at[k, 1, 0, a], zsend.at[k, 5], zrcv.at[k, 5], dev_zm),
        )

    def xf_copy(k):
        part = gown.reshape(NC, 4, 2, 256, 128).at[k, :, 1 - xh]
        return rdma(part, xf.at[k - NZ], xsend.at[k], xrcv.at[k], dev_x)

    def x_copy(k):
        return rdma(xs.at[k], xr.at[k], xsend.at[k], xrcv.at[k], dev_x)

    def spread_copy(k, d):
        yd = lax.rem(y + d, 4)
        return rdma(qs.at[k, :, pl.ds(yd * 32, 32)], w.at[k, y], wsend.at[k], wrcv.at[k], y_dev(d))

    def l_copies(k):
        own_part = full.at[k, :, mine_x, :, y]
        copies = [rdma(own_part, own_part, lsend.at[k, 0], lrcv.at[k, 0], dev_l)]
        for n, yy in enumerate((ym, yp, yo)):
            part = full.at[k, pl.ds(ZP, 4 - ZP), mine_x, :, yy]
            copies.append(rdma(part, part, lsend.at[k, n + 1], lrcv.at[k, n + 1], dev_l))
        return copies

    def y_copies(k):
        copies = []
        for n, x in enumerate((mine_x, 1 - mine_x)):
            groups = pl.ds(0, (4, ZP)[n])
            part = full.at[k, groups, x, :, y]
            below, above = full.at[k, groups, x, 0, ym], full.at[k, groups, x, 1, yp]
            copies += [
                rdma(part, part, ysend.at[k, 4 * n], yrcv.at[k, 4 * n], dev_yp),
                rdma(part, part, ysend.at[k, 4 * n + 1], yrcv.at[k, 4 * n + 1], dev_ym),
                rdma(below, below, ysend.at[k, 4 * n + 2], yrcv.at[k, 4 * n + 2], dev_yp),
                rdma(above, above, ysend.at[k, 4 * n + 3], yrcv.at[k, 4 * n + 3], dev_ym),
            ]
        return copies

    def sl_copy():
        part = sfull.at[:, mine_x]
        return rdma(part, part, ssend.at[2], srcv.at[2], dev_l)

    def hid_wait(n, _):
        for h in range(2):
            hid_load(n, h).wait()
        return 0

    def s_piece(p):
        n = p // 2
        q = lax.rem(p, 2)
        k = jnp.where(n < 4, n, jnp.where(n == 4, NZ, jnp.where(n == 5, 4, jnp.where(n == 6, NZ + 1, n - 2))))
        kb = k // 2
        row = lax.rem(k, 2) * 128

        @pl.when(p == 0)
        def _():
            hid_wait(0, 0)

        @pl.when(p == 2)
        def _():
            lax.fori_loop(1, NB, hid_wait, 0)
            for load in loads:
                load.start()

        @pl.when(q == 0)
        def _():
            first = pl.ds(pl.multiple_of(kb * 128, 128), 128)
            second = pl.ds(pl.multiple_of(HALF + kb * 128, 128), 128)
            hidt[pl.ds(0, 128), :] = hid[:, first].T
            hidt[pl.ds(128, 128), :] = hid[:, second].T

        def block(i):
            far = pl.ds(pl.multiple_of((2 * i + 1 - c) * 256 + row, 128), 128)
            near = pl.ds(pl.multiple_of((2 * i + c) * 256 + row, 128), 128)
            both = jnp.concatenate([go[:, far], go[:, near]], axis=1)
            return jnp.dot(hidt[...], both, preferred_element_type=F32).astype(BF16)

        def pair(j, _):
            i = 4 * q + 2 * j

            @pl.when(k == 0)
            def _():
                for b in range(4):
                    go_load(2 * i + b).wait()

            one, two = block(i), block(i + 1)
            goth[k, i] = one[:, :128]
            goth[k, i + 1] = two[:, :128]
            gown[k, i] = one[:, 128:]
            gown[k, i + 1] = two[:, 128:]
            core_copy(k, i).start()
            core_copy(k, i + 1).start()
            return 0

        lax.fori_loop(0, 2, pair, 0)

    def core_add(k):
        core_all(k).wait_recv()

        def add(i, _):
            gown[k, i] = (gown[k, i].astype(F32) + crecv[k, i].astype(F32)).astype(BF16)
            return 0

        lax.fori_loop(0, 8, add, 0)

    def s_zstart(k):
        @pl.when(k < NZ)
        def _():
            core_add(k)
            for copy in z_copies(k)[:2]:
                copy.start()

        @pl.when(k >= NZ)
        def _():
            xf_copy(k).wait_recv()

            def add(i, _):
                b = 2 * i + xh
                gown[k, b] = (gown[k, b].astype(F32) + xf[k - NZ, i].astype(F32)).astype(BF16)
                return 0

            lax.fori_loop(0, 4, add, 0)
            for copy in zx_copies(k)[:2]:
                copy.start()

    def s_xsend(k):
        core_add(k)
        xf_copy(k).start()

    def s_zfill(k):
        @pl.when(k < NZ)
        def _():
            for copy in z_copies(k)[2:4]:
                copy.start()

        @pl.when(k >= NZ)
        def _():
            for copy in zx_copies(k)[2:4]:
                copy.start()

    def s_zmid(k):
        sides = ((zp, pl.ds(128, 128)), (zm, pl.ds(0, 128)))

        @pl.when(k < NZ)
        def _():
            copies = z_copies(k)
            for n, (zi, rows) in enumerate(sides):
                copies[n].wait_recv()
                blocks = pl.ds(2 * zi, 2)
                gown[k, blocks, rows] = (gown[k, blocks, rows].astype(F32) + z1[k, n].astype(F32)).astype(BF16)
                copies[4 + n].start()

        @pl.when(k >= NZ)
        def _():
            copies = zx_copies(k)
            for n, (zi, rows) in enumerate(sides):
                copies[n].wait_recv()
                b = 2 * zi + xh
                gown[k, b, rows] = (gown[k, b, rows].astype(F32) + z1[k, n, 0].astype(F32)).astype(BF16)
                copies[4 + n].start()

    def s_zend(k):
        def total(q, slot):
            return gown[k, 2 * z + q].astype(F32) + z2[k, 0, slot].astype(F32) + z2[k, 1, slot].astype(F32)

        @pl.when(k < NZ)
        def _():
            for copy in z_copies(k)[2:]:
                copy.wait_recv()
            xs[k] = total(1 - xh, 1 - xh).astype(BF16)
            x_copy(k).start()
            own[lax.rem(k, 2)] = total(xh, xh)

        @pl.when(k >= NZ)
        def _():
            for copy in zx_copies(k)[2:]:
                copy.wait_recv()
            own[lax.rem(k, 2)] = total(xh, 0)
            xr[k] = jnp.zeros_like(xr[k])
            update(k)

    def s_update(k):
        @pl.when(k < NZ)
        def _():
            x_copy(k).wait_recv()
            update(k)

    def update(k):
        @pl.when(k == 0)
        def _():
            for load in loads:
                load.wait()

        fix_one = 1.0 - beta_one**steps_done
        fix_two = 1.0 - beta_two**steps_done
        kb = k // 2
        r = lax.rem(k, 2)
        rows = pl.ds(pl.multiple_of(r * 128, 128), 128)
        for h in range(2):
            cols = pl.ds(pl.multiple_of(h * HALF + kb * 128, 128), 128)
            grad_t = own[lax.rem(k, 2), pl.ds(h * 128, 128), :] + xr[k, pl.ds(h * 128, 128), :].astype(F32)
            grad = grad_t.T
            new_one = beta_one * m1[rows, cols] + (1.0 - beta_one) * grad
            new_two = beta_two * m2[rows, cols] + (1.0 - beta_two) * grad * grad
            new_master = ma[rows, cols] - learn_rate * (new_one / fix_one) / (
                jnp.sqrt(new_two / fix_two) + adam_eps
            )
            m1[rows, cols] = new_one
            m2[rows, cols] = new_two
            ma[rows, cols] = new_master
            peak = jnp.max(jnp.max(jnp.abs(new_master), axis=0, keepdims=True), axis=1, keepdims=True)
            scale = (peak + scale_eps).astype(BF16).astype(F32)
            qs[k, h] = (new_master / scale).astype(BF16)
            line = lax.broadcasted_iota(jnp.int32, (8, 128), 0)
            lane = lax.broadcasted_iota(jnp.int32, (8, 128), 1)
            here = jnp.logical_and(line == r, lane == kb)
            sacc[h] = jnp.where(here, jnp.broadcast_to(scale, (8, 128)), sacc[h])
        for d in range(1, 4):
            spread_copy(k, d).start()
        w[k, y] = qs[k, :, pl.ds(pl.multiple_of(y * 32, 32), 32), :]

        @pl.when(k == NC - 1)
        def _():
            for d in range(1, 4):
                rdma(sacc, ws.at[y], ssend.at[0], srcv.at[0], y_dev(d)).start()
            ws[y] = sacc[...]

    def spread_all(k):
        part = w.at[k, pl.ds(0, 3)]
        return rdma(part, part, wsend.at[k], wrcv.at[k], dev_yp)

    def spread_scales():
        part = ws.at[pl.ds(0, 3)]
        return rdma(part, part, ssend.at[0], srcv.at[0], dev_yp)

    def s_move(k):
        spread_all(k).wait_recv()

        @pl.when(k == NC - 1)
        def _():
            spread_scales().wait_recv()

        for ys in range(4):
            for h in range(2):
                fd, td = target(ys, h)
                here = jnp.logical_and(fd == f, td == t)

                @pl.when(jnp.logical_not(here))
                def _():
                    rdma(w.at[k, ys, h], full.at[k, z, xh, c, y], dsend.at[k], drcv.at[k], (fd, td)).start()

                @pl.when(here)
                def _():
                    full[k, z, xh, c, y] = w[k, ys, h]

                @pl.when(k == NC - 1)
                def _():
                    @pl.when(jnp.logical_not(here))
                    def _():
                        rdma(ws.at[ys, h], sfull.at[z, xh, c], ssend.at[1], srcv.at[1], (fd, td)).start()

                    @pl.when(here)
                    def _():
                        sfull[z, xh, c] = ws[ys, h]

    def move_wait(k, send):
        def wait(count):
            part = w.at[k].reshape(8, 32, 128).at[pl.ds(0, count)]
            copy = rdma(part, part, dsend.at[k], drcv.at[k], dev_core)
            copy.wait_send() if send else copy.wait_recv()

        @pl.when(is_self)
        def _():
            wait(7)

        @pl.when(jnp.logical_not(is_self))
        def _():
            wait(8)

    def scale_move_wait(send):
        def wait(count):
            part = ws.reshape(8, 8, 128).at[pl.ds(0, count)]
            copy = rdma(part, part, ssend.at[1], srcv.at[1], dev_core)
            copy.wait_send() if send else copy.wait_recv()

        @pl.when(is_self)
        def _():
            wait(7)

        @pl.when(jnp.logical_not(is_self))
        def _():
            wait(8)

    def s_pair(k):
        move_wait(k, False)
        for copy in y_copies(k)[:2]:
            copy.start()
        l_copies(k)[0].start()

        @pl.when(k == NC - 1)
        def _():
            scale_move_wait(False)
            sl_copy().start()

    def s_ymid(k):
        copies = y_copies(k)
        pairs = l_copies(k)
        for n in range(2):
            copies[n].wait_recv()
            copies[2 + n].start()
            pairs[1 + n].start()
        pairs[0].wait_recv()
        copies[4].start()
        copies[5].start()

    def s_yend(k):
        copies = y_copies(k)
        for n in (4, 5):
            copies[n].wait_recv()
            copies[2 + n].start()
        copies[2].wait_recv()
        copies[3].wait_recv()
        l_copies(k)[3].start()

    def s_store(k):
        copies = y_copies(k)
        for n in (6, 7):
            copies[n].wait_recv()
        for copy in l_copies(k)[1:]:
            copy.wait_recv()

        @pl.when(k == NC - 1)
        def _():
            sl_copy().wait_recv()
            for zs in range(4):
                for xs_ in range(2):
                    for cs in range(2):
                        sc_out[pl.ds(zs * 8 + xs_ * 4 + cs * 2, 2), :] = sfull[zs, xs_, cs, pl.ds(0, 2), :]

    order = (
        (0, s_zstart, 0, NC),
        (0, s_zfill, 0, NC),
        (3, s_zend, 0, NC),
        s_xsend,
        (4, s_move, NZ, NC),
        1,
        (7, s_pair, 0, NZ),
        (5, s_pair, NZ, NC),
        1,
        (1, s_zmid, 0, NC),
        (8, s_ymid, 0, NZ),
        (6, s_ymid, NZ, NC),
        1,
        (4, s_update, 0, NZ),
        (5, s_move, 0, NZ),
        (9, s_yend, 0, NZ),
        (7, s_yend, NZ, NC),
        (11, s_store, 0, NZ),
        (9, s_store, NZ, NC),
    )

    def first(p, _):
        s_piece(p)
        return 0

    lax.fori_loop(0, 2, first, 0)

    def step(n, _):
        ahead = 0
        for entry in order:
            if isinstance(entry, int):
                def some(m, _, start=2 + 3 * n + ahead):
                    @pl.when(start + m < 2 * NC)
                    def _():
                        s_piece(start + m)

                    return 0

                lax.fori_loop(0, entry, some, 0)
                ahead += entry
                continue
            if entry is s_xsend:
                for k, start in ((NZ, 4), (NZ + 1, 6)):

                    @pl.when(n == start)
                    def _():
                        entry(k)

                continue
            delay, stage, least, end = entry
            k = n - delay

            @pl.when(jnp.logical_and(k >= least, k < end))
            def _():
                stage(k)

        return 0

    lax.fori_loop(0, NC + 9, step, 0)

    def drain(k, _):
        core_all(k).wait_send()

        @pl.when(k < NZ)
        def _():
            for copy in z_copies(k):
                copy.wait_send()
            x_copy(k).wait_send()

        @pl.when(k >= NZ)
        def _():
            for copy in zx_copies(k):
                copy.wait_send()
            xf_copy(k).wait_send()

        spread_all(k).wait_send()
        move_wait(k, True)
        for copy in l_copies(k):
            copy.wait_send()
        for copy in y_copies(k):
            copy.wait_send()
        return 0

    lax.fori_loop(0, NC, drain, 0)
    spread_scales().wait_send()
    scale_move_wait(True)
    sl_copy().wait_send()


def store_kernel(ma, m1, m2, full, scales, ma_out, m1_out, m2_out, q_out, sc_out, sem):
    copies = [
        pltpu.make_async_copy(src, dst, sem.at[n])
        for n, (src, dst) in enumerate(((ma, ma_out), (m1, m1_out), (m2, m2_out)))
    ]
    for k in range(NC):
        copies.append(
            pltpu.make_async_copy(
                full.at[k].reshape(16, 128, 128),
                q_out.at[:, k % 2, :, pl.ds(k // 2 * 128, 128)],
                sem.at[3 + k],
            )
        )
    for copy in copies:
        copy.start()
    sc_out[...] = scales[...].T[:NB].astype(BF16)
    for copy in copies:
        copy.wait()


def local(hidden, grad_out, master, moment_one, moment_two):
    weights = pltpu.VMEM((256, 1792), F32)
    vmem = pltpu.VMEM
    dma = pltpu.SemaphoreType.DMA
    anyspace = pl.BlockSpec(memory_space=pl.ANY)
    new_master, new_one, new_two, quantized, scales = pl.pallas_call(
        kernel,
        out_shape=(
            weights,
            weights,
            weights,
            pltpu.VMEM((NC, 4, 2, 2, 4, 32, 128), BF16),
            pltpu.VMEM((32, 128), F32),
        ),
        in_specs=[anyspace] * 5,
        out_specs=(pl.BlockSpec(memory_space=pltpu.VMEM),) * 4 + (pl.BlockSpec(memory_space=pltpu.VMEM),),
        scratch_shapes=[
            vmem((1024, 1792), BF16),
            vmem((256, 1024), BF16),
            vmem((1024, 4096), BF16),
            vmem((NC, 8, 256, 128), BF16),
            vmem((NC, 8, 256, 128), BF16),
            vmem((NC, 8, 256, 128), BF16),
            vmem((NC, 2, 2, 128, 128), BF16),
            vmem((NC, 2, 2, 256, 128), BF16),
            vmem((2, 256, 128), F32),
            vmem((NC, 256, 128), BF16),
            vmem((NC, 256, 128), BF16),
            vmem((NC - NZ, 4, 256, 128), BF16),
            vmem((NC, 2, 128, 128), BF16),
            vmem((NC, 4, 2, 32, 128), BF16),
            vmem((2, 8, 128), F32),
            vmem((4, 2, 8, 128), F32),
            vmem((4, 2, 2, 8, 128), F32),
            dma((3,)),
            dma((NB, 2)),
            dma((16,)),
            dma((NC,)), dma((NC,)),
            dma((NC, 6)), dma((NC, 6)),
            dma((NC,)), dma((NC,)),
            dma((NC,)), dma((NC,)),
            dma((NC,)), dma((NC,)),
            dma((NC, 4)), dma((NC, 4)),
            dma((NC, 8)), dma((NC, 8)),
            dma((3,)), dma((3,)),
        ],
        compiler_params=pltpu.CompilerParams(
            collective_id=0, has_side_effects=True, vmem_limit_bytes=46 * 1024 * 1024
        ),
    )(hidden, grad_out, master, moment_one, moment_two)
    weights = jax.ShapeDtypeStruct((256, 1792), F32)
    *weights, quantized, scale = pl.pallas_call(
        store_kernel,
        out_shape=(
            weights,
            weights,
            weights,
            jax.ShapeDtypeStruct((16, 2, 128, HALF), BF16),
            jax.ShapeDtypeStruct((NB, 32), BF16),
        ),
        in_specs=[anyspace] * 4 + [pl.BlockSpec(memory_space=pltpu.VMEM)],
        out_specs=(anyspace,) * 4 + (pl.BlockSpec(memory_space=pltpu.VMEM),),
        scratch_shapes=[dma((3 + NC,))],
        compiler_params=pltpu.CompilerParams(vmem_limit_bytes=1024 * 1024),
    )(new_master, new_one, new_two, quantized, scales)
    return (*weights, quantized.reshape(4096, HALF), scale.T)


def solution(mesh):
    return jax.shard_map(
        local,
        mesh=mesh,
        in_specs=(
            P("fsdp", "tp"),
            P("fsdp", None),
            P("fsdp", "tp"),
            P("fsdp", "tp"),
            P("fsdp", "tp"),
        ),
        out_specs=(
            P("fsdp", "tp"),
            P("fsdp", "tp"),
            P("fsdp", "tp"),
            P(None, "fsdp"),
            P(None, "fsdp"),
        ),
        check_vma=False,
    )
```

```python
import functools

import jax
import jax.numpy as jnp
from jax import lax
from jax.experimental import pallas as pl
from jax.experimental.pallas import tpu as pltpu
from jax.sharding import PartitionSpec as P

beta_one = 0.9
beta_two = 0.95
learn_rate = 0.005
adam_eps = 1e-08
scale_eps = 1e-06
steps_done = 4

NB = 7
NC = 2 * NB
NZ = NC - 2
ZP = 2
HALF = 896
F32 = jnp.float32
BF16 = jnp.bfloat16
MESH = pl.DeviceIdType.MESH


def kernel(
    hid_in, go_in, ma_in, m1_in, m2_in,
    ma, m1, m2, full, sc_out,
    hid, hidt, go, gown, goth, crecv, z1, z2, own, xs, xr, xf, qs, w, sacc, ws, sfull,
    lsem, hsem, gsem, csend, crcv, zsend, zrcv, xsend, xrcv, wsend, wrcv, dsend, drcv,
    lsend, lrcv, ysend, yrcv, ssend, srcv,
):
    f = lax.axis_index("fsdp")
    t = lax.axis_index("tp")
    c = lax.rem(f, 2)
    g = f // 2
    xh = lax.rem(g, 2)
    z = g // 2
    y = lax.rem(t, 4)
    xl = t // 4
    zp, zm, zo = lax.rem(z + 1, 4), lax.rem(z + 3, 4), lax.rem(z + 2, 4)
    yp, ym, yo = lax.rem(y + 1, 4), lax.rem(y + 3, 4), lax.rem(y + 2, 4)
    dev_core = (f + 1 - 2 * c, t)
    dev_zp = (f + 4 * (zp - z), t)
    dev_zm = (f + 4 * (zm - z), t)
    dev_x = (f + 2 - 4 * xh, t)
    dev_l = (f, t + 4 - 8 * xl)
    dev_yp = (f, t + yp - y)
    dev_ym = (f, t + ym - y)
    xo = g // 4
    is_self = xo == xl
    mine_x = jnp.where(is_self, xh, 1 - xh)

    def y_dev(d):
        return (f, xl * 4 + lax.rem(y + d, 4))

    def target(ys, h):
        xd = jnp.where(xh == ys % 2, xl, 1 - xl)
        return (2 * (xl * 4 + ys) + h, xd * 4 + y)

    def go_load(b):
        cols = pl.ds(pl.multiple_of(b * 256, 256), 256)
        return pltpu.make_async_copy(go_in.at[:, cols], go.at[:, cols], gsem.at[b])

    def hid_load(n, h):
        cols = pl.ds(pl.multiple_of(h * HALF + n * 128, 128), 128)
        return pltpu.make_async_copy(hid_in.at[:, cols], hid.at[:, cols], hsem.at[n, h])

    loads = [
        pltpu.make_async_copy(ma_in, ma, lsem.at[0]),
        pltpu.make_async_copy(m1_in, m1, lsem.at[1]),
        pltpu.make_async_copy(m2_in, m2, lsem.at[2]),
    ]

    def start_go(b, _):
        go_load(b).start()
        return 0

    def start_hid(n, _):
        for h in range(2):
            hid_load(n, h).start()
        return 0

    start_hid(0, 0)
    lax.fori_loop(0, 16, start_go, 0)

    barrier = pltpu.get_barrier_semaphore()
    for dev in (dev_core, dev_zp, dev_zm, dev_x, dev_l, y_dev(1), y_dev(2), y_dev(3)):
        pl.semaphore_signal(barrier, inc=1, device_id=dev, device_id_type=MESH)
    for ys in range(4):
        for h in range(2):
            fd, td = target(ys, h)

            @pl.when(jnp.logical_not(jnp.logical_and(fd == f, td == t)))
            def _():
                pl.semaphore_signal(barrier, inc=1, device_id=(fd, td), device_id_type=MESH)

    for zs in range(4):
        for cs in range(2):
            fs, ts = 4 * zs + 2 * mine_x + cs, xo * 4 + y

            @pl.when(jnp.logical_not(jnp.logical_and(fs == f, ts == t)))
            def _():
                pl.semaphore_signal(barrier, inc=1, device_id=(fs, ts), device_id_type=MESH)

    @pl.when(is_self)
    def _():
        pl.semaphore_wait(barrier, 22)

    @pl.when(jnp.logical_not(is_self))
    def _():
        pl.semaphore_wait(barrier, 24)

    sacc[...] = jnp.zeros_like(sacc)
    lax.fori_loop(1, NB, start_hid, 0)

    def rdma(src, dst, send, recv, dev):
        return pltpu.make_async_remote_copy(
            src_ref=src, dst_ref=dst, send_sem=send, recv_sem=recv, device_id=dev, device_id_type=MESH
        )

    def core_copy(k, i):
        return rdma(goth.at[k, i], crecv.at[k, i], csend.at[k], crcv.at[k], dev_core)

    def core_all(k):
        return rdma(goth.at[k], crecv.at[k], csend.at[k], crcv.at[k], dev_core)

    def z_copies(k):
        a, b = pl.ds(0, 128), pl.ds(128, 128)
        far, up, down = pl.ds(2 * zo, 2), pl.ds(2 * zp, 2), pl.ds(2 * zm, 2)
        return (
            rdma(gown.at[k, far, b], z1.at[k, 0], zsend.at[k, 0], zrcv.at[k, 0], dev_zp),
            rdma(gown.at[k, far, a], z1.at[k, 1], zsend.at[k, 1], zrcv.at[k, 1], dev_zm),
            rdma(gown.at[k, up, a], z2.at[k, 0, :, a], zsend.at[k, 2], zrcv.at[k, 2], dev_zp),
            rdma(gown.at[k, down, b], z2.at[k, 1, :, b], zsend.at[k, 3], zrcv.at[k, 3], dev_zm),
            rdma(gown.at[k, up, b], z2.at[k, 0, :, b], zsend.at[k, 4], zrcv.at[k, 4], dev_zp),
            rdma(gown.at[k, down, a], z2.at[k, 1, :, a], zsend.at[k, 5], zrcv.at[k, 5], dev_zm),
        )

    def zx_copies(k):
        a, b = pl.ds(0, 128), pl.ds(128, 128)
        far, up, down = 2 * zo + xh, 2 * zp + xh, 2 * zm + xh
        return (
            rdma(gown.at[k, far, b], z1.at[k, 0, 0], zsend.at[k, 0], zrcv.at[k, 0], dev_zp),
            rdma(gown.at[k, far, a], z1.at[k, 1, 0], zsend.at[k, 1], zrcv.at[k, 1], dev_zm),
            rdma(gown.at[k, up, a], z2.at[k, 0, 0, a], zsend.at[k, 2], zrcv.at[k, 2], dev_zp),
            rdma(gown.at[k, down, b], z2.at[k, 1, 0, b], zsend.at[k, 3], zrcv.at[k, 3], dev_zm),
            rdma(gown.at[k, up, b], z2.at[k, 0, 0, b], zsend.at[k, 4], zrcv.at[k, 4], dev_zp),
            rdma(gown.at[k, down, a], z2.at[k, 1, 0, a], zsend.at[k, 5], zrcv.at[k, 5], dev_zm),
        )

    def xf_copy(k):
        part = gown.reshape(NC, 4, 2, 256, 128).at[k, :, 1 - xh]
        return rdma(part, xf.at[k - NZ], xsend.at[k], xrcv.at[k], dev_x)

    def x_copy(k):
        return rdma(xs.at[k], xr.at[k], xsend.at[k], xrcv.at[k], dev_x)

    def spread_copy(k, d):
        yd = lax.rem(y + d, 4)
        return rdma(qs.at[k, :, pl.ds(yd * 32, 32)], w.at[k, y], wsend.at[k], wrcv.at[k], y_dev(d))

    def l_copies(k):
        own_part = full.at[k, :, mine_x, :, y]
        copies = [rdma(own_part, own_part, lsend.at[k, 0], lrcv.at[k, 0], dev_l)]
        for n, yy in enumerate((ym, yp, yo)):
            part = full.at[k, pl.ds(ZP, 4 - ZP), mine_x, :, yy]
            copies.append(rdma(part, part, lsend.at[k, n + 1], lrcv.at[k, n + 1], dev_l))
        return copies

    def y_copies(k):
        copies = []
        for n, x in enumerate((mine_x, 1 - mine_x)):
            groups = pl.ds(0, (4, ZP)[n])
            part = full.at[k, groups, x, :, y]
            below, above = full.at[k, groups, x, 0, ym], full.at[k, groups, x, 1, yp]
            copies += [
                rdma(part, part, ysend.at[k, 4 * n], yrcv.at[k, 4 * n], dev_yp),
                rdma(part, part, ysend.at[k, 4 * n + 1], yrcv.at[k, 4 * n + 1], dev_ym),
                rdma(below, below, ysend.at[k, 4 * n + 2], yrcv.at[k, 4 * n + 2], dev_yp),
                rdma(above, above, ysend.at[k, 4 * n + 3], yrcv.at[k, 4 * n + 3], dev_ym),
            ]
        return copies

    def sl_copy():
        part = sfull.at[:, mine_x]
        return rdma(part, part, ssend.at[2], srcv.at[2], dev_l)

    def hid_wait(n, _):
        for h in range(2):
            hid_load(n, h).wait()
        return 0

    def s_piece(p):
        n = p // 2
        q = lax.rem(p, 2)
        k = jnp.where(n < 4, n, jnp.where(n == 4, NZ, jnp.where(n == 5, 4, jnp.where(n == 6, NZ + 1, n - 2))))
        kb = k // 2
        row = lax.rem(k, 2) * 128

        @pl.when(p == 0)
        def _():
            hid_wait(0, 0)

        @pl.when(p == 2)
        def _():
            lax.fori_loop(1, NB, hid_wait, 0)
            for load in loads:
                load.start()

        @pl.when(q == 0)
        def _():
            first = pl.ds(pl.multiple_of(kb * 128, 128), 128)
            second = pl.ds(pl.multiple_of(HALF + kb * 128, 128), 128)
            hidt[pl.ds(0, 128), :] = hid[:, first].T
            hidt[pl.ds(128, 128), :] = hid[:, second].T

        def block(i):
            far = pl.ds(pl.multiple_of((2 * i + 1 - c) * 256 + row, 128), 128)
            near = pl.ds(pl.multiple_of((2 * i + c) * 256 + row, 128), 128)
            both = jnp.concatenate([go[:, far], go[:, near]], axis=1)
            return jnp.dot(hidt[...], both, preferred_element_type=F32).astype(BF16)

        def pair(j, _):
            i = 4 * q + 2 * j

            @pl.when(k == 0)
            def _():
                for b in range(4):
                    go_load(2 * i + b).wait()

            one, two = block(i), block(i + 1)
            goth[k, i] = one[:, :128]
            goth[k, i + 1] = two[:, :128]
            gown[k, i] = one[:, 128:]
            gown[k, i + 1] = two[:, 128:]
            core_copy(k, i).start()
            core_copy(k, i + 1).start()
            return 0

        lax.fori_loop(0, 2, pair, 0)

    def core_add(k):
        core_all(k).wait_recv()

        def add(i, _):
            gown[k, i] = (gown[k, i].astype(F32) + crecv[k, i].astype(F32)).astype(BF16)
            return 0

        lax.fori_loop(0, 8, add, 0)

    def s_zstart(k):
        @pl.when(k < NZ)
        def _():
            core_add(k)
            for copy in z_copies(k)[:2]:
                copy.start()

        @pl.when(k >= NZ)
        def _():
            xf_copy(k).wait_recv()

            def add(i, _):
                b = 2 * i + xh
                gown[k, b] = (gown[k, b].astype(F32) + xf[k - NZ, i].astype(F32)).astype(BF16)
                return 0

            lax.fori_loop(0, 4, add, 0)
            for copy in zx_copies(k)[:2]:
                copy.start()

    def s_xsend(k):
        core_add(k)
        xf_copy(k).start()

    def s_zfill(k):
        @pl.when(k < NZ)
        def _():
            for copy in z_copies(k)[2:4]:
                copy.start()

        @pl.when(k >= NZ)
        def _():
            for copy in zx_copies(k)[2:4]:
                copy.start()

    def s_zmid(k):
        sides = ((zp, pl.ds(128, 128)), (zm, pl.ds(0, 128)))

        @pl.when(k < NZ)
        def _():
            copies = z_copies(k)
            for n, (zi, rows) in enumerate(sides):
                copies[n].wait_recv()
                blocks = pl.ds(2 * zi, 2)
                gown[k, blocks, rows] = (gown[k, blocks, rows].astype(F32) + z1[k, n].astype(F32)).astype(BF16)
                copies[4 + n].start()

        @pl.when(k >= NZ)
        def _():
            copies = zx_copies(k)
            for n, (zi, rows) in enumerate(sides):
                copies[n].wait_recv()
                b = 2 * zi + xh
                gown[k, b, rows] = (gown[k, b, rows].astype(F32) + z1[k, n, 0].astype(F32)).astype(BF16)
                copies[4 + n].start()

    def s_zend(k):
        def total(q, slot):
            return gown[k, 2 * z + q].astype(F32) + z2[k, 0, slot].astype(F32) + z2[k, 1, slot].astype(F32)

        @pl.when(k < NZ)
        def _():
            for copy in z_copies(k)[2:]:
                copy.wait_recv()
            xs[k] = total(1 - xh, 1 - xh).astype(BF16)
            x_copy(k).start()
            own[lax.rem(k, 2)] = total(xh, xh)

        @pl.when(k >= NZ)
        def _():
            for copy in zx_copies(k)[2:]:
                copy.wait_recv()
            own[lax.rem(k, 2)] = total(xh, 0)
            xr[k] = jnp.zeros_like(xr[k])
            update(k)

    def s_update(k):
        @pl.when(k < NZ)
        def _():
            x_copy(k).wait_recv()
            update(k)

    def update(k):
        @pl.when(k == 0)
        def _():
            for load in loads:
                load.wait()

        fix_one = 1.0 - beta_one**steps_done
        fix_two = 1.0 - beta_two**steps_done
        kb = k // 2
        r = lax.rem(k, 2)
        rows = pl.ds(pl.multiple_of(r * 128, 128), 128)
        for h in range(2):
            cols = pl.ds(pl.multiple_of(h * HALF + kb * 128, 128), 128)
            grad_t = own[lax.rem(k, 2), pl.ds(h * 128, 128), :] + xr[k, pl.ds(h * 128, 128), :].astype(F32)
            grad = grad_t.T
            new_one = beta_one * m1[rows, cols] + (1.0 - beta_one) * grad
            new_two = beta_two * m2[rows, cols] + (1.0 - beta_two) * grad * grad
            new_master = ma[rows, cols] - learn_rate * (new_one / fix_one) / (
                jnp.sqrt(new_two / fix_two) + adam_eps
            )
            m1[rows, cols] = new_one
            m2[rows, cols] = new_two
            ma[rows, cols] = new_master
            peak = jnp.max(jnp.max(jnp.abs(new_master), axis=0, keepdims=True), axis=1, keepdims=True)
            scale = (peak + scale_eps).astype(BF16).astype(F32)
            qs[k, h] = (new_master / scale).astype(BF16)
            line = lax.broadcasted_iota(jnp.int32, (8, 128), 0)
            lane = lax.broadcasted_iota(jnp.int32, (8, 128), 1)
            here = jnp.logical_and(line == r, lane == kb)
            sacc[h] = jnp.where(here, jnp.broadcast_to(scale, (8, 128)), sacc[h])
        for d in range(1, 4):
            spread_copy(k, d).start()
        w[k, y] = qs[k, :, pl.ds(pl.multiple_of(y * 32, 32), 32), :]

        @pl.when(k == NC - 1)
        def _():
            for d in range(1, 4):
                rdma(sacc, ws.at[y], ssend.at[0], srcv.at[0], y_dev(d)).start()
            ws[y] = sacc[...]

    def spread_all(k):
        part = w.at[k, pl.ds(0, 3)]
        return rdma(part, part, wsend.at[k], wrcv.at[k], dev_yp)

    def spread_scales():
        part = ws.at[pl.ds(0, 3)]
        return rdma(part, part, ssend.at[0], srcv.at[0], dev_yp)

    def s_move(k):
        spread_all(k).wait_recv()

        @pl.when(k == NC - 1)
        def _():
            spread_scales().wait_recv()

        for ys in range(4):
            for h in range(2):
                fd, td = target(ys, h)
                here = jnp.logical_and(fd == f, td == t)

                @pl.when(jnp.logical_not(here))
                def _():
                    rdma(w.at[k, ys, h], full.at[k, z, xh, c, y], dsend.at[k], drcv.at[k], (fd, td)).start()

                @pl.when(here)
                def _():
                    full[k, z, xh, c, y] = w[k, ys, h]

                @pl.when(k == NC - 1)
                def _():
                    @pl.when(jnp.logical_not(here))
                    def _():
                        rdma(ws.at[ys, h], sfull.at[z, xh, c], ssend.at[1], srcv.at[1], (fd, td)).start()

                    @pl.when(here)
                    def _():
                        sfull[z, xh, c] = ws[ys, h]

    def move_wait(k, send):
        def wait(count):
            part = w.at[k].reshape(8, 32, 128).at[pl.ds(0, count)]
            copy = rdma(part, part, dsend.at[k], drcv.at[k], dev_core)
            copy.wait_send() if send else copy.wait_recv()

        @pl.when(is_self)
        def _():
            wait(7)

        @pl.when(jnp.logical_not(is_self))
        def _():
            wait(8)

    def scale_move_wait(send):
        def wait(count):
            part = ws.reshape(8, 8, 128).at[pl.ds(0, count)]
            copy = rdma(part, part, ssend.at[1], srcv.at[1], dev_core)
            copy.wait_send() if send else copy.wait_recv()

        @pl.when(is_self)
        def _():
            wait(7)

        @pl.when(jnp.logical_not(is_self))
        def _():
            wait(8)

    def s_pair(k):
        move_wait(k, False)
        for copy in y_copies(k)[:2]:
            copy.start()
        l_copies(k)[0].start()

        @pl.when(k == NC - 1)
        def _():
            scale_move_wait(False)
            sl_copy().start()

    def s_ymid(k):
        copies = y_copies(k)
        pairs = l_copies(k)
        for n in range(2):
            copies[n].wait_recv()
            copies[2 + n].start()
            pairs[1 + n].start()
        pairs[0].wait_recv()
        copies[4].start()
        copies[5].start()

    def s_yend(k):
        copies = y_copies(k)
        for n in (4, 5):
            copies[n].wait_recv()
            copies[2 + n].start()
        copies[2].wait_recv()
        copies[3].wait_recv()
        l_copies(k)[3].start()

    def s_store(k):
        copies = y_copies(k)
        for n in (6, 7):
            copies[n].wait_recv()
        for copy in l_copies(k)[1:]:
            copy.wait_recv()

        @pl.when(k == NC - 1)
        def _():
            sl_copy().wait_recv()
            for zs in range(4):
                for xs_ in range(2):
                    for cs in range(2):
                        sc_out[pl.ds(zs * 8 + xs_ * 4 + cs * 2, 2), :] = sfull[zs, xs_, cs, pl.ds(0, 2), :]

    def s_drain(k):
        core_all(k).wait_send()

        @pl.when(k < NZ)
        def _():
            for copy in z_copies(k):
                copy.wait_send()
            x_copy(k).wait_send()

        @pl.when(k >= NZ)
        def _():
            for copy in zx_copies(k):
                copy.wait_send()
            xf_copy(k).wait_send()

        spread_all(k).wait_send()
        move_wait(k, True)
        for copy in l_copies(k):
            copy.wait_send()
        for copy in y_copies(k):
            copy.wait_send()

    order = (
        (0, s_zstart, 0, NC),
        (0, s_zfill, 0, NC),
        (3, s_zend, 0, NC),
        s_xsend,
        (4, s_move, NZ, NC),
        1,
        (7, s_pair, 0, NZ),
        (5, s_pair, NZ, NC),
        1,
        (1, s_zmid, 0, NC),
        (8, s_ymid, 0, NZ),
        (6, s_ymid, NZ, NC),
        1,
        (4, s_update, 0, NZ),
        (5, s_move, 0, NZ),
        (9, s_yend, 0, NZ),
        (7, s_yend, NZ, NC),
        (11, s_store, 0, NZ),
        (9, s_store, NZ, NC),
        (11, s_drain, 0, NZ),
        (9, s_drain, NZ, NC),
    )

    def first(p, _):
        s_piece(p)
        return 0

    lax.fori_loop(0, 2, first, 0)

    def step(n, _):
        ahead = 0
        for entry in order:
            if isinstance(entry, int):
                def some(m, _, start=2 + 3 * n + ahead):
                    @pl.when(start + m < 2 * NC)
                    def _():
                        s_piece(start + m)

                    return 0

                lax.fori_loop(0, entry, some, 0)
                ahead += entry
                continue
            if entry is s_xsend:
                for k, start in ((NZ, 4), (NZ + 1, 6)):

                    @pl.when(n == start)
                    def _():
                        entry(k)

                continue
            delay, stage, least, end = entry
            k = n - delay

            @pl.when(jnp.logical_and(k >= least, k < end))
            def _():
                stage(k)

        return 0

    lax.fori_loop(0, NC + 9, step, 0)

    spread_scales().wait_send()
    scale_move_wait(True)
    sl_copy().wait_send()


def store_kernel(ma, m1, m2, full, scales, ma_out, m1_out, m2_out, q_out, sc_out, sem):
    copies = [
        pltpu.make_async_copy(src, dst, sem.at[n])
        for n, (src, dst) in enumerate(((ma, ma_out), (m1, m1_out), (m2, m2_out)))
    ]
    for k in range(NC):
        copies.append(
            pltpu.make_async_copy(
                full.at[k].reshape(16, 128, 128),
                q_out.at[:, k % 2, :, pl.ds(k // 2 * 128, 128)],
                sem.at[3 + k],
            )
        )
    for copy in copies:
        copy.start()
    sc_out[...] = scales[...].T[:NB].astype(BF16)
    for copy in copies:
        copy.wait()


def local(hidden, grad_out, master, moment_one, moment_two):
    weights = pltpu.VMEM((256, 1792), F32)
    vmem = pltpu.VMEM
    dma = pltpu.SemaphoreType.DMA
    anyspace = pl.BlockSpec(memory_space=pl.ANY)
    new_master, new_one, new_two, quantized, scales = pl.pallas_call(
        kernel,
        out_shape=(
            weights,
            weights,
            weights,
            pltpu.VMEM((NC, 4, 2, 2, 4, 32, 128), BF16),
            pltpu.VMEM((32, 128), F32),
        ),
        in_specs=[anyspace] * 5,
        out_specs=(pl.BlockSpec(memory_space=pltpu.VMEM),) * 4 + (pl.BlockSpec(memory_space=pltpu.VMEM),),
        scratch_shapes=[
            vmem((1024, 1792), BF16),
            vmem((256, 1024), BF16),
            vmem((1024, 4096), BF16),
            vmem((NC, 8, 256, 128), BF16),
            vmem((NC, 8, 256, 128), BF16),
            vmem((NC, 8, 256, 128), BF16),
            vmem((NC, 2, 2, 128, 128), BF16),
            vmem((NC, 2, 2, 256, 128), BF16),
            vmem((2, 256, 128), F32),
            vmem((NC, 256, 128), BF16),
            vmem((NC, 256, 128), BF16),
            vmem((NC - NZ, 4, 256, 128), BF16),
            vmem((NC, 2, 128, 128), BF16),
            vmem((NC, 4, 2, 32, 128), BF16),
            vmem((2, 8, 128), F32),
            vmem((4, 2, 8, 128), F32),
            vmem((4, 2, 2, 8, 128), F32),
            dma((3,)),
            dma((NB, 2)),
            dma((16,)),
            dma((NC,)), dma((NC,)),
            dma((NC, 6)), dma((NC, 6)),
            dma((NC,)), dma((NC,)),
            dma((NC,)), dma((NC,)),
            dma((NC,)), dma((NC,)),
            dma((NC, 4)), dma((NC, 4)),
            dma((NC, 8)), dma((NC, 8)),
            dma((3,)), dma((3,)),
        ],
        compiler_params=pltpu.CompilerParams(
            collective_id=0, has_side_effects=True, vmem_limit_bytes=46 * 1024 * 1024
        ),
    )(hidden, grad_out, master, moment_one, moment_two)
    weights = jax.ShapeDtypeStruct((256, 1792), F32)
    *weights, quantized, scale = pl.pallas_call(
        store_kernel,
        out_shape=(
            weights,
            weights,
            weights,
            jax.ShapeDtypeStruct((16, 2, 128, HALF), BF16),
            jax.ShapeDtypeStruct((NB, 32), BF16),
        ),
        in_specs=[anyspace] * 4 + [pl.BlockSpec(memory_space=pltpu.VMEM)],
        out_specs=(anyspace,) * 4 + (pl.BlockSpec(memory_space=pltpu.VMEM),),
        scratch_shapes=[dma((3 + NC,))],
        compiler_params=pltpu.CompilerParams(vmem_limit_bytes=1024 * 1024),
    )(new_master, new_one, new_two, quantized, scales)
    return (*weights, quantized.reshape(4096, HALF), scale.T)


def solution(mesh):
    return jax.shard_map(
        local,
        mesh=mesh,
        in_specs=(
            P("fsdp", "tp"),
            P("fsdp", None),
            P("fsdp", "tp"),
            P("fsdp", "tp"),
            P("fsdp", "tp"),
        ),
        out_specs=(
            P("fsdp", "tp"),
            P("fsdp", "tp"),
            P("fsdp", "tp"),
            P(None, "fsdp"),
            P(None, "fsdp"),
        ),
        check_vma=False,
    )
```
